16 devices in a mesh: sp: 16 (over z, y, x, core).
Axes of the slice: x: 2, y: 2, z: 2, core: 2. Of those that a mesh axis runs over, the one named last changes fastest.
Arguments:
- hidden: bfloat16 [32, 512, 1024], P(None, 'sp')
- norm_gain: float32 [1024], replicated
- w_q: bfloat16 [1024, 2048], replicated
- w_k: bfloat16 [1024, 1024], replicated
- w_v: bfloat16 [1024, 1024], replicated
- q_gain: float32 [128], replicated
- k_gain: float32 [128], replicated
- w_o: bfloat16 [2048, 1024], replicated
- d_out: bfloat16 [32, 512, 1024], P(None, 'sp')
Outputs:
- output 1: bfloat16 [32, 512, 1024], P(None, 'sp')
- output 2: bfloat16 [32, 512, 1024], P(None, 'sp')
- output 3: float32 [1024, 2048], replicated
- output 4: float32 [1024, 1024], replicated
- output 5: float32 [1024, 1024], replicated
- output 6: float32 [2048, 1024], replicated
- output 7: float32 [1024], replicated
- output 8: float32 [128], replicated
- output 9: float32 [128], replicated
All inputs are finite; a program needn't handle non-finite values.
Results may differ from the reference program's by a relative error of at most 0.0181044.
Values are sent between devices in bfloat16 or wider.
A program may use at most 1 GiB of HBM per device.

```python
import math
import jax
import jax.numpy as jnp
from jax import lax

BATCH_SIZE = 32
SEQ_LEN = 512
MODEL_DIM = 1024
Q_HEADS = 16
KV_HEADS = 8
HEAD_DIM = 128
ROPE_BASE = 1000000
NORM_EPS = 1e-6


def setup_inputs(seed: int = 0) -> dict:
    keys = jax.random.split(jax.random.key(seed), 9)
    q_width = Q_HEADS * HEAD_DIM
    kv_width = KV_HEADS * HEAD_DIM
    hidden = jax.random.normal(keys[0], (BATCH_SIZE, SEQ_LEN, MODEL_DIM), jnp.float32)
    norm_gain = 1.0 + 0.5 * jax.random.normal(keys[1], (MODEL_DIM,), jnp.float32)
    w_q = jax.random.normal(keys[2], (MODEL_DIM, q_width), jnp.float32) * MODEL_DIM ** -0.5
    w_k = jax.random.normal(keys[3], (MODEL_DIM, kv_width), jnp.float32) * MODEL_DIM ** -0.5
    w_v = jax.random.normal(keys[4], (MODEL_DIM, kv_width), jnp.float32) * MODEL_DIM ** -0.5
    q_gain = 1.0 + 0.3 * jax.random.normal(keys[5], (HEAD_DIM,), jnp.float32)
    k_gain = 1.0 + 0.3 * jax.random.normal(keys[6], (HEAD_DIM,), jnp.float32)
    w_o = jax.random.normal(keys[7], (q_width, MODEL_DIM), jnp.float32) * q_width ** -0.5
    d_out = jax.random.normal(keys[8], (BATCH_SIZE, SEQ_LEN, MODEL_DIM), jnp.float32)
    return {'hidden': hidden.astype(jnp.bfloat16), 'norm_gain': norm_gain, 'w_q': w_q.astype(jnp.bfloat16), 'w_k': w_k.astype(jnp.bfloat16), 'w_v': w_v.astype(jnp.bfloat16), 'q_gain': q_gain, 'k_gain': k_gain, 'w_o': w_o.astype(jnp.bfloat16), 'd_out': d_out.astype(jnp.bfloat16)}


def rms_scale(values, gain):
    return values * lax.rsqrt(jnp.mean(values * values, axis=-1, keepdims=True) + NORM_EPS) * gain


def rope_tables(positions):
    half_dim = HEAD_DIM // 2
    inv_freq = jnp.exp(jnp.arange(half_dim).astype(jnp.float32) * (-2.0 * math.log(ROPE_BASE) / HEAD_DIM))
    angles = positions[:, None] * inv_freq[None, :]
    return jnp.cos(angles), jnp.sin(angles)


def qk_post(raw, gain, cos_tab, sin_tab):
    normed = rms_scale(raw, gain)
    half_dim = HEAD_DIM // 2
    first = normed[..., :half_dim]
    second = normed[..., half_dim:]
    cos_b = cos_tab[None, :, None, :]
    sin_b = sin_tab[None, :, None, :]
    return jnp.concatenate([first * cos_b - second * sin_b, second * cos_b + first * sin_b], axis=-1)


def head_attn(q_head, k_head, v_head):
    n_pos = q_head.shape[1]
    scores = jnp.einsum('bqd,bkd->bqk', q_head, k_head) * HEAD_DIM ** -0.5
    causal = jnp.arange(n_pos)[:, None] >= jnp.arange(n_pos)[None, :]
    scores = jnp.where(causal[None], scores, -1e30)
    attn_prob = jax.nn.softmax(scores, axis=-1)
    attn_prob = attn_prob + lax.stop_gradient(attn_prob.astype(jnp.bfloat16).astype(jnp.float32) - attn_prob)
    return jnp.einsum('bqk,bkd->bqd', attn_prob, v_head)


def reference(hidden, norm_gain, w_q, w_k, w_v, q_gain, k_gain, w_o, d_out):
    group_size = Q_HEADS // KV_HEADS
    tokens = BATCH_SIZE * SEQ_LEN
    hidden_f = hidden.astype(jnp.float32)
    normed_f, norm_back = jax.vjp(rms_scale, hidden_f, norm_gain)
    flat_norm = normed_f.astype(jnp.bfloat16).reshape(tokens, MODEL_DIM)
    q_raw = jnp.dot(flat_norm, w_q, preferred_element_type=jnp.float32).astype(jnp.bfloat16)
    k_raw = jnp.dot(flat_norm, w_k, preferred_element_type=jnp.float32).astype(jnp.bfloat16)
    v_raw = jnp.dot(flat_norm, w_v, preferred_element_type=jnp.float32).astype(jnp.bfloat16)
    cos_tab, sin_tab = rope_tables(jnp.arange(SEQ_LEN).astype(jnp.float32))

    def post_both(q_in, k_in, q_scale, k_scale):
        return qk_post(q_in, q_scale, cos_tab, sin_tab), qk_post(k_in, k_scale, cos_tab, sin_tab)

    (q_rot, k_rot), post_back = jax.vjp(post_both, q_raw.astype(jnp.float32).reshape(BATCH_SIZE, SEQ_LEN, Q_HEADS, HEAD_DIM), k_raw.astype(jnp.float32).reshape(BATCH_SIZE, SEQ_LEN, KV_HEADS, HEAD_DIM), q_gain, k_gain)
    q_heads = jnp.moveaxis(q_rot.astype(jnp.bfloat16), 2, 0)
    k_heads = jnp.moveaxis(k_rot.astype(jnp.bfloat16), 2, 0)
    v_heads = jnp.moveaxis(v_raw.reshape(BATCH_SIZE, SEQ_LEN, KV_HEADS, HEAD_DIM), 2, 0)
    head_ids = jnp.arange(Q_HEADS)

    def fwd_one(head_item):
        q_head, head_id = head_item
        kv_id = head_id // group_size
        return head_attn(q_head.astype(jnp.float32), k_heads[kv_id].astype(jnp.float32), v_heads[kv_id].astype(jnp.float32))

    out_heads = lax.map(fwd_one, (q_heads, head_ids))
    attn = jnp.moveaxis(out_heads, 0, 2).astype(jnp.bfloat16).reshape(tokens, Q_HEADS * HEAD_DIM)
    y_out = (hidden_f.reshape(tokens, MODEL_DIM) + jnp.dot(attn, w_o, preferred_element_type=jnp.float32)).astype(jnp.bfloat16).reshape(BATCH_SIZE, SEQ_LEN, MODEL_DIM)
    dy_flat = d_out.reshape(tokens, MODEL_DIM)
    d_attn = jnp.dot(dy_flat, w_o.T, preferred_element_type=jnp.float32).astype(jnp.bfloat16)
    d_wo = jnp.dot(attn.T, dy_flat, preferred_element_type=jnp.float32)
    d_attn_heads = jnp.moveaxis(d_attn.reshape(BATCH_SIZE, SEQ_LEN, Q_HEADS, HEAD_DIM), 2, 0)

    def bwd_one(head_item):
        q_head, d_head, head_id = head_item
        kv_id = head_id // group_size
        _, head_back = jax.vjp(head_attn, q_head.astype(jnp.float32), k_heads[kv_id].astype(jnp.float32), v_heads[kv_id].astype(jnp.float32))
        return head_back(d_head.astype(jnp.float32))

    dq_heads, dk_each, dv_each = lax.map(bwd_one, (q_heads, d_attn_heads, head_ids))
    dk_heads = jnp.sum(dk_each.reshape(KV_HEADS, group_size, BATCH_SIZE, SEQ_LEN, HEAD_DIM), axis=1)
    dv_heads = jnp.sum(dv_each.reshape(KV_HEADS, group_size, BATCH_SIZE, SEQ_LEN, HEAD_DIM), axis=1)
    dq_all = jnp.moveaxis(dq_heads, 0, 2).astype(jnp.bfloat16)
    dk_all = jnp.moveaxis(dk_heads, 0, 2).astype(jnp.bfloat16)
    dv_flat = jnp.moveaxis(dv_heads, 0, 2).astype(jnp.bfloat16).reshape(tokens, KV_HEADS * HEAD_DIM)
    dq_raw_f, dk_raw_f, d_qgain, d_kgain = post_back((dq_all.astype(jnp.float32), dk_all.astype(jnp.float32)))
    dq_raw = dq_raw_f.astype(jnp.bfloat16).reshape(tokens, Q_HEADS * HEAD_DIM)
    dk_raw = dk_raw_f.astype(jnp.bfloat16).reshape(tokens, KV_HEADS * HEAD_DIM)
    d_wq = jnp.dot(flat_norm.T, dq_raw, preferred_element_type=jnp.float32)
    d_wk = jnp.dot(flat_norm.T, dk_raw, preferred_element_type=jnp.float32)
    d_wv = jnp.dot(flat_norm.T, dv_flat, preferred_element_type=jnp.float32)
    d_normed = jnp.dot(dq_raw, w_q.T, preferred_element_type=jnp.float32) + jnp.dot(dk_raw, w_k.T, preferred_element_type=jnp.float32) + jnp.dot(dv_flat, w_v.T, preferred_element_type=jnp.float32)
    dx_f, d_ngain = norm_back(d_normed.reshape(BATCH_SIZE, SEQ_LEN, MODEL_DIM))
    d_hidden = (d_out.astype(jnp.float32) + dx_f).astype(jnp.bfloat16)
    return (y_out, d_hidden, d_wq, d_wk, d_wv, d_wo, d_ngain, d_qgain, d_kgain)
```

```python
import math
import jax
import jax.numpy as jnp
from jax import lax
from jax.experimental import pallas as pl
from jax.experimental.pallas import tpu as pltpu
from jax.sharding import PartitionSpec as P

ROPE_BASE = 1000000.0
NORM_EPS = 1e-6
LOG2E = 1.4426950408889634
F32 = jnp.float32
BF16 = jnp.bfloat16
QBLK = 256
VMEM_LIMIT = 60 * 1024 * 1024


def dot(a, b, ca, cb):
    return lax.dot_general(a, b, (((ca,), (cb,)), ((), ())), preferred_element_type=F32)


def rope_tables(n_pos, head_dim):
    half_dim = head_dim // 2
    inv_freq = jnp.exp(jnp.arange(half_dim).astype(F32) * (-2.0 * math.log(ROPE_BASE) / head_dim))
    angles = jnp.arange(n_pos).astype(F32)[:, None] * inv_freq[None, :]
    cos, sin = jnp.cos(angles), jnp.sin(angles)
    return jnp.concatenate([cos, cos], axis=-1), jnp.concatenate([-sin, sin], axis=-1)


def norm_rope(raw, gain, cos, sin):
    inv = lax.rsqrt(jnp.mean(raw * raw, axis=-1, keepdims=True) + NORM_EPS)
    normed = raw * inv * gain
    return normed * cos + pltpu.roll(normed, raw.shape[-1] // 2, 1) * sin


def norm_rope_back(d_rot, raw, gain, cos, sin):
    inv = lax.rsqrt(jnp.mean(raw * raw, axis=-1, keepdims=True) + NORM_EPS)
    unit = raw * inv
    d_normed = d_rot * cos - pltpu.roll(d_rot, raw.shape[-1] // 2, 1) * sin
    d_gain = jnp.sum(d_normed * unit, axis=0, keepdims=True)
    d_unit = d_normed * gain
    d_raw = inv * (d_unit - unit * jnp.mean(d_unit * unit, axis=-1, keepdims=True))
    return d_raw, d_gain


def causal_mask_t(scores_t, first_q):
    n_key, n_q = scores_t.shape
    key = lax.broadcasted_iota(jnp.int32, (n_q, n_q), 0)
    query = lax.broadcasted_iota(jnp.int32, (n_q, n_q), 1)
    diag = jnp.where(query >= key, scores_t[first_q:], -1e30)
    if first_q == 0:
        return diag
    return jnp.concatenate([scores_t[:first_q], diag], axis=0)


def fwd_kernel(x_ref, gain_ref, wq_ref, wk_ref, wv_ref, qg_ref, kg_ref, cos_ref, sin_ref,
               h_ref, qraw_ref, kraw_ref, qrot_ref, krot_ref, v_ref, o_ref, lse_ref):
    n_src, _, n_loc, dim = x_ref.shape
    n_pos = n_src * n_loc
    head_dim = qg_ref.shape[-1]
    group = wq_ref.shape[1] // head_dim

    @pl.when(pl.program_id(1) == 0)
    def _():
        x = x_ref[:, 0].reshape(n_pos, dim).astype(F32)
        inv = lax.rsqrt(jnp.mean(x * x, axis=-1, keepdims=True) + NORM_EPS)
        h_ref[:, 0] = (x * inv * gain_ref[...]).astype(BF16).reshape(n_src, n_loc, dim)

    h = h_ref[:, 0].reshape(n_pos, dim)
    cos, sin = cos_ref[...], sin_ref[...]
    q_raw = dot(h, wq_ref[...], 1, 0).astype(BF16)
    k_raw = dot(h, wk_ref[...], 1, 0).astype(BF16)
    v = dot(h, wv_ref[...], 1, 0).astype(BF16)
    qraw_ref[0] = q_raw
    kraw_ref[0] = k_raw
    v_ref[0] = v
    k_rot = norm_rope(k_raw.astype(F32), kg_ref[...], cos, sin).astype(BF16)
    krot_ref[0] = k_rot
    scale = head_dim ** -0.5 * LOG2E
    for j in range(group):
        cols = slice(j * head_dim, (j + 1) * head_dim)
        q_rot = norm_rope(q_raw[:, cols].astype(F32), qg_ref[...], cos, sin).astype(BF16)
        qrot_ref[0, :, cols] = q_rot
        for first in range(0, n_pos, QBLK):
            n_key = first + QBLK
            scores = causal_mask_t(dot(k_rot[:n_key], q_rot[first:n_key], 1, 1) * scale, first)
            top = jnp.max(scores, axis=0, keepdims=True)
            e = jnp.exp2(scores - top)
            total = jnp.sum(e, axis=0, keepdims=True)
            prob = (e * (1.0 / total)).astype(BF16)
            lse_ref[0, 0, j:j + 1, first:n_key] = top + jnp.log2(total)
            o_blk = dot(prob, v[:n_key], 0, 0).astype(BF16)
            o_ref[first // n_loc:n_key // n_loc, 0, :, cols] = o_blk.reshape(QBLK // n_loc, n_loc, head_dim)


def bwd_kernel(dy_ref, wo_ref, qraw_ref, kraw_ref, qrot_ref, krot_ref, v_ref, lse_ref, qg_ref, kg_ref, cos_ref, sin_ref,
               dq_ref, dk_ref, dv_ref, dqg_ref, dkg_ref):
    n_src, _, n_loc, dim = dy_ref.shape
    n_pos = n_src * n_loc
    head_dim = qg_ref.shape[-1]
    group = wo_ref.shape[0] // head_dim

    @pl.when((pl.program_id(0) == 0) & (pl.program_id(1) == 0))
    def _():
        dqg_ref[...] = jnp.zeros_like(dqg_ref)
        dkg_ref[...] = jnp.zeros_like(dkg_ref)

    cos, sin = cos_ref[...], sin_ref[...]
    scale = head_dim ** -0.5
    d_o = dot(dy_ref[:, 0].reshape(n_pos, dim), wo_ref[...], 1, 1).astype(BF16)
    k_rot, v = krot_ref[0], v_ref[0]
    dk_sum = [jnp.zeros((QBLK, head_dim), F32) for _ in range(n_pos // QBLK)]
    dv_sum = [jnp.zeros((QBLK, head_dim), F32) for _ in range(n_pos // QBLK)]
    for j in range(group):
        cols = slice(j * head_dim, (j + 1) * head_dim)
        dq_parts = []
        for first in range(0, n_pos, QBLK):
            n_key = first + QBLK
            q_blk = qrot_ref[0, first:n_key, cols]
            do_blk = d_o[first:n_key, cols]
            scores = causal_mask_t(dot(k_rot[:n_key], q_blk, 1, 1) * (scale * LOG2E), first)
            prob = jnp.exp2(scores - lse_ref[0, 0, j:j + 1, first:n_key])
            d_prob = dot(v[:n_key], do_blk, 1, 1)
            inner = jnp.sum(prob * d_prob, axis=0, keepdims=True)
            d_scores = (prob * (d_prob - inner) * scale).astype(BF16)
            dv_blk = dot(prob.astype(BF16), do_blk, 1, 0)
            dk_blk = dot(d_scores, q_blk, 1, 0)
            for i in range(n_key // QBLK):
                dv_sum[i] += dv_blk[i * QBLK:(i + 1) * QBLK]
                dk_sum[i] += dk_blk[i * QBLK:(i + 1) * QBLK]
            dq_parts.append(dot(d_scores, k_rot[:n_key], 0, 0))
        dq = jnp.concatenate(dq_parts, axis=0).astype(BF16).astype(F32)
        dq_raw, d_gain = norm_rope_back(dq, qraw_ref[0, :, cols].astype(F32), qg_ref[...], cos, sin)
        dq_ref[:, 0, :, cols] = dq_raw.astype(BF16).reshape(n_src, n_loc, head_dim)
        dqg_ref[...] += d_gain
    dk = jnp.concatenate(dk_sum, axis=0).astype(BF16).astype(F32)
    dk_raw, d_gain = norm_rope_back(dk, kraw_ref[0].astype(F32), kg_ref[...], cos, sin)
    dk_ref[:, 0] = dk_raw.astype(BF16).reshape(n_src, n_loc, head_dim)
    dkg_ref[...] += d_gain
    dv_ref[:, 0] = jnp.concatenate(dv_sum, axis=0).astype(BF16).reshape(n_src, n_loc, head_dim)


def attention_fwd(x, norm_gain, w_q, w_k, w_v, q_gain, k_gain, cos, sin):
    n_src, rows, n_loc, dim = x.shape
    n_pos, head_dim = cos.shape
    kv_heads = w_k.shape[1] // head_dim
    group = w_q.shape[1] // w_k.shape[1]
    qw = group * head_dim
    seq = lambda width: pl.BlockSpec((1, n_pos, width), lambda r, g: (r, 0, g))
    const = lambda shape: pl.BlockSpec(shape, lambda r, g: (0, 0))
    weight = lambda width: pl.BlockSpec((dim, width), lambda r, g: (0, g))
    return pl.pallas_call(
        fwd_kernel,
        grid=(rows, kv_heads),
        in_specs=[
            pl.BlockSpec((n_src, 1, n_loc, dim), lambda r, g: (0, r, 0, 0)), const((1, dim)),
            weight(qw), weight(head_dim), weight(head_dim), const((1, head_dim)), const((1, head_dim)),
            const((n_pos, head_dim)), const((n_pos, head_dim))],
        out_specs=[
            pl.BlockSpec((n_src, 1, n_loc, dim), lambda r, g: (0, r, 0, 0)),
            seq(qw), seq(head_dim), seq(qw), seq(head_dim), seq(head_dim),
            pl.BlockSpec((n_src, 1, n_loc, qw), lambda r, g: (0, r, 0, g)),
            pl.BlockSpec((1, 1, group, n_pos), lambda r, g: (r, g, 0, 0))],
        out_shape=[
            jax.ShapeDtypeStruct(x.shape, BF16),
            jax.ShapeDtypeStruct((rows, n_pos, kv_heads * qw), BF16),
            jax.ShapeDtypeStruct((rows, n_pos, kv_heads * head_dim), BF16),
            jax.ShapeDtypeStruct((rows, n_pos, kv_heads * qw), BF16),
            jax.ShapeDtypeStruct((rows, n_pos, kv_heads * head_dim), BF16),
            jax.ShapeDtypeStruct((rows, n_pos, kv_heads * head_dim), BF16),
            jax.ShapeDtypeStruct((n_src, rows, n_loc, kv_heads * qw), BF16),
            jax.ShapeDtypeStruct((rows, kv_heads, group, n_pos), F32)],
        compiler_params=pltpu.CompilerParams(
            dimension_semantics=('arbitrary', 'arbitrary'), vmem_limit_bytes=VMEM_LIMIT),
        cost_estimate=pl.CostEstimate(flops=12 * 10**9, bytes_accessed=50 * 10**6, transcendentals=0),
        name='attn_fwd',
    )(x, norm_gain[None], w_q, w_k, w_v, q_gain[None], k_gain[None], cos, sin)


def attention_bwd(d_y, w_o, q_raw, k_raw, q_rot, k_rot, v, lse, q_gain, k_gain, cos, sin):
    n_src, rows, n_loc, dim = d_y.shape
    n_pos, head_dim = cos.shape
    _, kv_heads, group, _ = lse.shape
    qw = group * head_dim
    seq = lambda width: pl.BlockSpec((1, n_pos, width), lambda r, g: (r, 0, g))
    const = lambda shape: pl.BlockSpec(shape, lambda r, g: (0, 0))
    out = lambda width: pl.BlockSpec((n_src, 1, n_loc, width), lambda r, g: (0, r, 0, g))
    return pl.pallas_call(
        bwd_kernel,
        grid=(rows, kv_heads),
        in_specs=[
            pl.BlockSpec((n_src, 1, n_loc, dim), lambda r, g: (0, r, 0, 0)),
            pl.BlockSpec((qw, dim), lambda r, g: (g, 0)),
            seq(qw), seq(head_dim), seq(qw), seq(head_dim), seq(head_dim),
            pl.BlockSpec((1, 1, group, n_pos), lambda r, g: (r, g, 0, 0)),
            const((1, head_dim)), const((1, head_dim)), const((n_pos, head_dim)), const((n_pos, head_dim))],
        out_specs=[out(qw), out(head_dim), out(head_dim), const((1, head_dim)), const((1, head_dim))],
        out_shape=[
            jax.ShapeDtypeStruct((n_src, rows, n_loc, kv_heads * qw), BF16),
            jax.ShapeDtypeStruct((n_src, rows, n_loc, kv_heads * head_dim), BF16),
            jax.ShapeDtypeStruct((n_src, rows, n_loc, kv_heads * head_dim), BF16),
            jax.ShapeDtypeStruct((1, head_dim), F32),
            jax.ShapeDtypeStruct((1, head_dim), F32)],
        compiler_params=pltpu.CompilerParams(
            dimension_semantics=('arbitrary', 'arbitrary'), vmem_limit_bytes=VMEM_LIMIT),
        cost_estimate=pl.CostEstimate(flops=14 * 10**9, bytes_accessed=50 * 10**6, transcendentals=0),
        name='attn_bwd',
    )(d_y, w_o, q_raw, k_raw, q_rot, k_rot, v, lse, q_gain[None], k_gain[None], cos, sin)


def solution(mesh):
    n_dev = mesh.shape['sp']
    seq_spec = P(None, 'sp', None)
    replicated = P()

    def local_step(hidden, norm_gain, w_q, w_k, w_v, q_gain, k_gain, w_o, d_out):
        n_batch, n_loc, dim = hidden.shape
        head_dim = q_gain.shape[0]
        rows = n_batch // n_dev
        tokens = rows * n_loc * n_dev
        cos, sin = rope_tables(n_loc * n_dev, head_dim)

        def exchange(a):
            return lax.all_to_all(a.reshape(n_dev, rows, n_loc, dim), 'sp', 0, 0, tiled=True)

        x = exchange(hidden)
        d_y = exchange(d_out)
        h, q_raw, k_raw, q_rot, k_rot, v, o, lse = attention_fwd(x, norm_gain, w_q, w_k, w_v, q_gain, k_gain, cos, sin)
        o = o.reshape(tokens, -1)
        h = h.reshape(tokens, dim)
        dy_flat = d_y.reshape(tokens, dim)
        x_f = x.reshape(tokens, dim).astype(F32)
        d_wo = lax.psum(dot(o, dy_flat, 0, 0), 'sp')
        y = (x_f + dot(o, w_o, 1, 0)).astype(BF16)
        y_out = exchange(y).reshape(n_batch, n_loc, dim)
        dq, dk, dv, d_qg, d_kg = attention_bwd(d_y, w_o, q_raw, k_raw, q_rot, k_rot, v, lse, q_gain, k_gain, cos, sin)
        dq = dq.reshape(tokens, -1)
        dk = dk.reshape(tokens, -1)
        dv = dv.reshape(tokens, -1)
        d_normed = dot(dq, w_q, 1, 1) + dot(dk, w_k, 1, 1) + dot(dv, w_v, 1, 1)
        inv = lax.rsqrt(jnp.mean(x_f * x_f, axis=-1, keepdims=True) + NORM_EPS)
        unit = x_f * inv
        d_ng = jnp.sum(d_normed * unit, axis=0)
        d_unit = d_normed * norm_gain
        d_x = inv * (d_unit - unit * jnp.mean(d_unit * unit, axis=-1, keepdims=True))
        d_hidden = exchange((dy_flat.astype(F32) + d_x).astype(BF16)).reshape(n_batch, n_loc, dim)
        d_wq = dot(h, dq, 0, 0)
        d_wk = dot(h, dk, 0, 0)
        d_wv = dot(h, dv, 0, 0)
        late, d_wo = lax.optimization_barrier(((d_wq, d_wk, d_wv, d_ng, d_qg[0], d_kg[0]), d_wo))
        d_wq, d_wk, d_wv, d_ng, d_qg, d_kg = lax.psum(late, 'sp')
        return y_out, d_hidden, d_wq, d_wk, d_wv, d_wo, d_ng, d_qg, d_kg

    return jax.shard_map(local_step, mesh=mesh, in_specs=(seq_spec, replicated, replicated, replicated, replicated, replicated, replicated, replicated, seq_spec), out_specs=(seq_spec, seq_spec, replicated, replicated, replicated, replicated, replicated, replicated, replicated), check_vma=False)
```

```python
import math
import jax
import jax.numpy as jnp
import numpy as np
from jax import lax
from jax.experimental import pallas as pl
from jax.experimental.pallas import tpu as pltpu
from jax.sharding import PartitionSpec as P

ROPE_BASE = 1000000.0
NORM_EPS = 1e-6
LOG2E = 1.4426950408889634
F32 = jnp.float32
BF16 = jnp.bfloat16
QBLK = 256
VMEM_LIMIT = 67043328
COLOURS = ((1, 2, 3), (2, 3, 1), (3, 1, 2))


def dot(a, b, ca, cb):
    return lax.dot_general(a, b, (((ca,), (cb,)), ((), ())), preferred_element_type=F32)


def rope_tables(n_pos, head_dim):
    half_dim = head_dim // 2
    inv_freq = np.exp(np.arange(half_dim, dtype=np.float32) * np.float32(-2.0 * math.log(ROPE_BASE) / head_dim))
    angles = np.arange(n_pos, dtype=np.float32)[:, None] * inv_freq[None, :]
    cos, sin = np.cos(angles), np.sin(angles)
    return np.concatenate([cos, cos], axis=-1), np.concatenate([-sin, sin], axis=-1)


def norm_rope(raw, gain, cos, sin):
    inv = lax.rsqrt(jnp.mean(raw * raw, axis=-1, keepdims=True) + NORM_EPS)
    unit = raw * inv
    normed = unit * gain
    return normed * cos + pltpu.roll(normed, raw.shape[-1] // 2, 1) * sin, unit, inv


def norm_rope_back(d_rot, unit, inv, gain, cos, sin):
    d_normed = d_rot * cos - pltpu.roll(d_rot, unit.shape[-1] // 2, 1) * sin
    d_gain = jnp.sum(d_normed * unit, axis=0, keepdims=True)
    d_unit = d_normed * gain
    return inv * (d_unit - unit * jnp.mean(d_unit * unit, axis=-1, keepdims=True)), d_gain


def causal_mask_t(scores_t, first_q):
    n_q = scores_t.shape[1]
    key = lax.broadcasted_iota(jnp.int32, (n_q, n_q), 0)
    query = lax.broadcasted_iota(jnp.int32, (n_q, n_q), 1)
    diag = jnp.where(query >= key, scores_t[first_q:], -1e30)
    if first_q == 0:
        return diag
    return jnp.concatenate([scores_t[:first_q], diag], axis=0)


def block_kernel(n_groups, hid_ref, dyin_ref, gain_ref, wq_ref, wk_ref, wv_ref, wo_ref, qg_ref, kg_ref, cos_ref, sin_ref,
                 y_ref, dx_ref, dwq_ref, dwk_ref, dwv_ref, dwo_ref, small_ref,
                 xs, dys, hs, ht, wcat, dqkv, oall, y_acc, dn_acc, u, r0, r1, r2, r3, r4, sm, smr,
                 in_send, in_recv, in_loc, d_send, d_recv, p_send, p_recv, g_send, g_recv, e_send, e_recv,
                 s_send, s_recv, o_sem, out_send, out_recv, out_loc):
    n_dev, rows, n_loc, dim = hid_ref.shape
    n_pos = n_dev * n_loc
    head_dim = qg_ref.shape[-1]
    qw = wq_ref.shape[1]
    group = qw // head_dim
    width = qw + 2 * head_dim
    half = u.shape[1] // 2
    blk = half // 3
    step = pl.program_id(0)
    me = lax.axis_index('sp')
    bit = [(me // (1 << i)) % 2 for i in range(4)]
    partner = [me + (1 << i) * (1 - 2 * bit[i]) for i in range(4)]

    def remote(src, dst, send, recv, device):
        return pltpu.make_async_remote_copy(src_ref=src, dst_ref=dst, send_sem=send, recv_sem=recv,
                                            device_id=(device,), device_id_type=pl.DeviceIdType.MESH)

    def rows_of(g, start, size):
        return u.at[g, pl.ds(pl.multiple_of(start, 32), size)]

    own, other = bit[0] * half, (1 - bit[0]) * half
    keep1, send1, keep2, send2, keep3, send3 = [], [], [], [], [], []
    for c, (d1, d2, d3) in enumerate(COLOURS):
        base = own + c * blk
        keep1.append(base + bit[d1] * (blk // 2))
        send1.append(base + (1 - bit[d1]) * (blk // 2))
        keep2.append(keep1[c] + bit[d2] * (blk // 4))
        send2.append(keep1[c] + (1 - bit[d2]) * (blk // 4))
        keep3.append(keep2[c] + bit[d3] * (blk // 8))
        send3.append(keep2[c] + (1 - bit[d3]) * (blk // 8))

    def core_scatter(g):
        return remote(rows_of(g, other, half), r0.at[g % 2], d_send.at[g % 2], d_recv.at[g % 2], partner[0])

    def scatter(phase, c, g):
        start, size, buf = ((send1, blk // 2, r1), (send2, blk // 4, r2), (send3, blk // 8, r3))[phase]
        return remote(rows_of(g, start[c], size), buf.at[g % 2, c], p_send.at[phase, c, g % 2], p_recv.at[phase, c, g % 2],
                      partner[COLOURS[c][phase]])

    def gather(phase, c, g):
        start, size = ((keep3, blk // 8), (keep2, blk // 4), (keep1, blk // 2))[phase]
        part = rows_of(g, start[c], size)
        return remote(part, part if phase else r4.at[g % 2, c], g_send.at[phase, c, g % 2], g_recv.at[phase, c, g % 2], partner[COLOURS[c][2 - phase]])

    def core_gather(g):
        part = rows_of(g, own, half)
        return remote(part, part, e_send.at[g % 2], e_recv.at[g % 2], partner[0])

    def out_copies(g):
        part = u.at[g]
        col = lambda n: pl.ds(pl.multiple_of(g * n, 128), n)
        orow = pl.ds(pl.multiple_of(g * qw, 128), qw)
        pieces = ((part.at[:dim, :qw], dwq_ref.at[:, col(qw)]),
                  (part.at[:dim, qw:qw + head_dim], dwk_ref.at[:, col(head_dim)]),
                  (part.at[:dim, qw + head_dim:], dwv_ref.at[:, col(head_dim)]),
                  (part.at[dim:dim + qw], dwo_ref.at[orow, :width]),
                  (part.at[dim + qw:], dwo_ref.at[orow, width:]))
        return [pltpu.make_async_copy(a, b, o_sem.at[i]) for i, (a, b) in enumerate(pieces)]

    def add_rows(g, start, size, buf):
        s = pl.ds(pl.multiple_of(start, 32), size)
        u[g, s] = u[g, s] + buf

    def stage(k, g):
        slot = g % 2
        if k == 1:
            core_scatter(g).wait()
            for c in range(3):
                add_rows(g, own + c * blk, blk, r0[slot, c * blk:(c + 1) * blk])
                scatter(0, c, g).start()
        elif k in (2, 3, 4):
            keep, size, buf = ((keep1, blk // 2, r1), (keep2, blk // 4, r2), (keep3, blk // 8, r3))[k - 2]
            for c in range(3):
                scatter(k - 2, c, g).wait()
            for c in range(3):
                add_rows(g, keep[c], size, buf[slot, c])
                (scatter(k - 1, c, g) if k < 4 else gather(0, c, g)).start()
        elif k in (5, 6):
            for c in range(3):
                gather(k - 5, c, g).wait()
            for c in range(3):
                if k == 5:
                    u[g, pl.ds(pl.multiple_of(send3[c], 32), blk // 8)] = r4[slot, c]
                gather(k - 4, c, g).start()
        elif k == 7:
            for c in range(3):
                gather(2, c, g).wait()
            core_gather(g).start()
        else:
            core_gather(g).wait()

            @pl.when(g > 0)
            def _():
                for copy in out_copies(g - 1):
                    copy.wait()
            for copy in out_copies(g):
                copy.start()

    def handler(sub):
        for k in range(8, 0, -1):
            if (sub - 2 - k) % 3 == 0:
                g = step + (sub - 2 - k) // 3

                @pl.when((g >= 0) & (g < n_groups))
                def _():
                    stage(k, g)
        for i in range(5):
            if i % 3 == sub:
                @pl.when(step == n_groups + i // 3)
                def _():
                    if i == 0:
                        small_copy(0).start()
                    else:
                        small_step(i - 1)

    def small_copy(i):
        return remote(sm.at[i], smr.at[i], s_send.at[i], s_recv.at[i], partner[i])

    def small_step(i):
        small_copy(i).wait()
        sm[i + 1] = sm[i] + smr[i]
        if i < 3:
            small_copy(i + 1).start()
        else:
            small_ref[...] = sm[4]

    def in_copy(which, row, peer):
        src, dst = (hid_ref, xs) if which == 0 else (dyin_ref, dys)
        n = 2 * row + which
        return remote(src.at[peer, row], dst.at[row, me], in_send.at[n], in_recv.at[n], peer)

    def in_local(which, row):
        src, dst = (hid_ref, xs) if which == 0 else (dyin_ref, dys)
        return pltpu.make_async_copy(src.at[me, row], dst.at[row, me], in_loc.at[2 * row + which])

    def in_wait(which, row):
        dst = xs if which == 0 else dys
        n = 2 * row + which
        many = dst.at[row, pl.ds(0, n_dev - 1)]
        pltpu.make_async_copy(many, many, in_recv.at[n]).wait()
        in_local(which, row).wait()

    def in_wait_send(which, row):
        many = (xs if which == 0 else dys).at[row, pl.ds(0, n_dev - 1)]
        pltpu.make_async_copy(many, many, in_send.at[2 * row + which]).wait()

    def out_copy(which, row, peer):
        src, dst = (xs, y_ref) if which == 0 else (dys, dx_ref)
        n = 2 * row + which
        return remote(src.at[row, peer], dst.at[me, row], out_send.at[n], out_recv.at[n], peer)

    def out_local(which, row):
        src, dst = (xs, y_ref) if which == 0 else (dys, dx_ref)
        return pltpu.make_async_copy(src.at[row, me], dst.at[me, row], out_loc.at[2 * row + which])

    def to_peers(make, which, row):
        def body(d, carry):
            make(which, row, lax.rem(me + d, n_dev)).start()
            return carry
        lax.fori_loop(1, n_dev, body, 0)

    @pl.when(step == 0)
    def _():
        barrier = pltpu.get_barrier_semaphore()

        def greet(d, carry):
            pl.semaphore_signal(barrier, inc=1, device_id=(lax.rem(me + d, n_dev),), device_id_type=pl.DeviceIdType.MESH)
            return carry
        lax.fori_loop(1, n_dev, greet, 0)
        pl.semaphore_wait(barrier, n_dev - 1)
        for row in range(rows):
            for which in range(2):
                in_local(which, row).start()
                to_peers(in_copy, which, row)
        y_acc[...] = jnp.zeros_like(y_acc)
        dn_acc[...] = jnp.zeros_like(dn_acc)
        sm[0] = jnp.zeros_like(sm[0])

    def tokens_of(row):
        return slice(row * n_pos, (row + 1) * n_pos)

    def row_compute(row):
        tok = tokens_of(row)
        cos, sin = cos_ref[...], sin_ref[...]
        scale = head_dim ** -0.5
        qkv = dot(hs[tok], wcat[...], 1, 0).astype(BF16)
        d_o = dot(dys[row].reshape(n_pos, dim), wo_ref[...], 1, 1).astype(BF16)
        k_rot, k_unit, k_inv = norm_rope(qkv[:, qw:qw + head_dim].astype(F32), kg_ref[...], cos, sin)
        k_rot = k_rot.astype(BF16)
        v = qkv[:, qw + head_dim:]
        dk_sum = [jnp.zeros((QBLK, head_dim), F32) for _ in range(n_pos // QBLK)]
        dv_sum = [jnp.zeros((QBLK, head_dim), F32) for _ in range(n_pos // QBLK)]
        for j in range(group):
            cols = slice(j * head_dim, (j + 1) * head_dim)
            q_rot, q_unit, q_inv = norm_rope(qkv[:, cols].astype(F32), qg_ref[...], cos, sin)
            q_rot = q_rot.astype(BF16)
            dq_parts = []
            for first in range(0, n_pos, QBLK):
                n_key = first + QBLK
                q_blk = q_rot[first:n_key]
                do_blk = d_o[first:n_key, cols]
                scores = causal_mask_t(dot(k_rot[:n_key], q_blk, 1, 1) * (scale * LOG2E), first)
                e = jnp.exp2(scores - jnp.max(scores, axis=0, keepdims=True))
                prob = e * (1.0 / jnp.sum(e, axis=0, keepdims=True))
                prob_bf = prob.astype(BF16)
                oall[row * n_pos + first:row * n_pos + n_key, cols] = dot(prob_bf, v[:n_key], 0, 0).astype(BF16)
                d_prob = dot(v[:n_key], do_blk, 1, 1)
                inner = jnp.sum(prob * d_prob, axis=0, keepdims=True)
                d_scores = (prob * (d_prob - inner) * scale).astype(BF16)
                dv_blk = dot(prob_bf, do_blk, 1, 0)
                dk_blk = dot(d_scores, q_blk, 1, 0)
                for i in range(n_key // QBLK):
                    dv_sum[i] += dv_blk[i * QBLK:(i + 1) * QBLK]
                    dk_sum[i] += dk_blk[i * QBLK:(i + 1) * QBLK]
                dq_parts.append(dot(d_scores, k_rot[:n_key], 0, 0))
            dq = jnp.concatenate(dq_parts, axis=0).astype(BF16).astype(F32)
            dq_raw, d_gain = norm_rope_back(dq, q_unit, q_inv, qg_ref[...], cos, sin)
            dqkv[tok, cols] = dq_raw.astype(BF16)
            sm[0, 1:2, :head_dim] += d_gain
        dk = jnp.concatenate(dk_sum, axis=0).astype(BF16).astype(F32)
        dk_raw, d_gain = norm_rope_back(dk, k_unit, k_inv, kg_ref[...], cos, sin)
        dqkv[tok, qw:qw + head_dim] = dk_raw.astype(BF16)
        sm[0, 1:2, head_dim:2 * head_dim] += d_gain
        dqkv[tok, qw + head_dim:] = jnp.concatenate(dv_sum, axis=0).astype(BF16)

    def input_norm(row):
        x = xs[row].reshape(n_pos, dim).astype(F32)
        inv = lax.rsqrt(jnp.mean(x * x, axis=-1, keepdims=True) + NORM_EPS)
        h = (x * inv * gain_ref[...]).astype(BF16)
        hs[tokens_of(row)] = h
        ht[:, tokens_of(row)] = h.T

    def finish_row(row):
        tok = tokens_of(row)
        x = xs[row].reshape(n_pos, dim).astype(F32)
        inv = lax.rsqrt(jnp.mean(x * x, axis=-1, keepdims=True) + NORM_EPS)
        unit = x * inv
        d_normed = dn_acc[tok]
        sm[0, 0:1] += jnp.sum(d_normed * unit, axis=0, keepdims=True)
        d_unit = d_normed * gain_ref[...]
        d_x = inv * (d_unit - unit * jnp.mean(d_unit * unit, axis=-1, keepdims=True))
        d_y = dys[row].reshape(n_pos, dim).astype(F32)
        dys[row] = (d_y + d_x).astype(BF16).reshape(n_dev, n_loc, dim)
        xs[row] = (x + y_acc[tok]).astype(BF16).reshape(n_dev, n_loc, dim)

    computing = step < n_groups

    @pl.when(computing)
    def _():
        wcat[:, :qw] = wq_ref[...]
        wcat[:, qw:qw + head_dim] = wk_ref[...]
        wcat[:, qw + head_dim:] = wv_ref[...]

    for row in range(rows):
        handler(row)

        @pl.when(step == 0)
        def _():
            in_wait(0, row)
            input_norm(row)
            in_wait(1, row)

        @pl.when(computing)
        def _():
            row_compute(row)

    handler(2)

    @pl.when(computing)
    def _():
        u[step, :dim] = dot(ht[...], dqkv[...], 1, 0)
        d_wo = dot(oall[...], dys[...].reshape(rows * n_pos, dim), 0, 0)
        u[step, dim:dim + qw] = d_wo[:, :width]
        u[step, dim + qw:] = d_wo[:, width:]
        core_scatter(step).start()
        y_acc[...] += dot(oall[...], wo_ref[...], 1, 0)
        dn_acc[...] += dot(dqkv[...], wcat[...], 1, 1)

    @pl.when(step == n_groups - 1)
    def _():
        for row in range(rows):
            for which in range(2):
                in_wait_send(which, row)
        for row in range(rows):
            finish_row(row)
            for which in (1, 0):
                out_local(which, row).start()
                to_peers(out_copy, which, row)

    @pl.when(step == pl.num_programs(0) - 1)
    def _():
        for copy in out_copies(n_groups - 1):
            copy.wait()
        for row in range(rows):
            for which in range(2):
                n = 2 * row + which
                many = (xs if which == 0 else dys).at[row, pl.ds(0, n_dev - 1)]
                landed = (y_ref if which == 0 else dx_ref).at[pl.ds(0, n_dev - 1), row]
                pltpu.make_async_copy(many, many, out_send.at[n]).wait()
                pltpu.make_async_copy(landed, landed, out_recv.at[n]).wait()
                out_local(which, row).wait()


def solution(mesh):
    n_dev = mesh.shape['sp']
    seq_spec = P(None, 'sp', None)
    replicated = P()

    def local_step(hidden, norm_gain, w_q, w_k, w_v, q_gain, k_gain, w_o, d_out):
        n_batch, n_loc, dim = hidden.shape
        head_dim = q_gain.shape[0]
        kv_heads = w_k.shape[1] // head_dim
        qw = w_q.shape[1] // kv_heads
        width = qw + 2 * head_dim
        rows = n_batch // n_dev
        n_pos = n_loc * n_dev
        tokens = rows * n_pos
        cos, sin = rope_tables(n_pos, head_dim)
        slice_rows = dim + 2 * qw
        blk = slice_rows // 6
        last = lambda t: jnp.minimum(t, kv_heads - 1)
        const = lambda shape: pl.BlockSpec(shape, lambda t: (0, 0))
        anywhere = pl.BlockSpec(memory_space=pl.ANY)
        act = (n_dev, rows, n_loc, dim)
        dma = pltpu.SemaphoreType.DMA
        y, d_hidden, d_wq, d_wk, d_wv, d_wo, small = pl.pallas_call(
            lambda *refs: block_kernel(kv_heads, *refs),
            grid=(kv_heads + 3,),
            in_specs=[
                anywhere, anywhere, const((1, dim)),
                pl.BlockSpec((dim, qw), lambda t: (0, last(t))),
                pl.BlockSpec((dim, head_dim), lambda t: (0, last(t))),
                pl.BlockSpec((dim, head_dim), lambda t: (0, last(t))),
                pl.BlockSpec((qw, dim), lambda t: (last(t), 0)),
                const((1, head_dim)), const((1, head_dim)), const((n_pos, head_dim)), const((n_pos, head_dim))],
            out_specs=[anywhere] * 6 + [const((8, dim))],
            out_shape=[
                jax.ShapeDtypeStruct(act, BF16), jax.ShapeDtypeStruct(act, BF16),
                jax.ShapeDtypeStruct(w_q.shape, F32), jax.ShapeDtypeStruct(w_k.shape, F32),
                jax.ShapeDtypeStruct(w_v.shape, F32), jax.ShapeDtypeStruct(w_o.shape, F32),
                jax.ShapeDtypeStruct((8, dim), F32)],
            scratch_shapes=[
                pltpu.VMEM((rows, n_dev, n_loc, dim), BF16), pltpu.VMEM((rows, n_dev, n_loc, dim), BF16),
                pltpu.VMEM((tokens, dim), BF16), pltpu.VMEM((dim, tokens), BF16),
                pltpu.VMEM((dim, width), BF16), pltpu.VMEM((tokens, width), BF16), pltpu.VMEM((tokens, qw), BF16),
                pltpu.VMEM((tokens, dim), F32), pltpu.VMEM((tokens, dim), F32),
                pltpu.VMEM((kv_heads, slice_rows, width), F32),
                pltpu.VMEM((2, slice_rows // 2, width), F32), pltpu.VMEM((2, 3, blk // 2, width), F32),
                pltpu.VMEM((2, 3, blk // 4, width), F32), pltpu.VMEM((2, 3, blk // 8, width), F32),
                pltpu.VMEM((2, 3, blk // 8, width), F32),
                pltpu.VMEM((5, 8, dim), F32), pltpu.VMEM((4, 8, dim), F32),
                dma((4,)), dma((4,)), dma((4,)), dma((2,)), dma((2,)), dma((3, 3, 2)), dma((3, 3, 2)),
                dma((3, 3, 2)), dma((3, 3, 2)), dma((2,)), dma((2,)), dma((4,)), dma((4,)), dma((5,)),
                dma((4,)), dma((4,)), dma((4,))],
            compiler_params=pltpu.CompilerParams(
                dimension_semantics=('arbitrary',), vmem_limit_bytes=VMEM_LIMIT, collective_id=0, has_side_effects=True),
            cost_estimate=pl.CostEstimate(flops=52 * 10**9, bytes_accessed=50 * 10**6, transcendentals=0),
            name='attn_block',
        )(hidden.reshape(act), d_out.reshape(act), norm_gain[None], w_q, w_k, w_v, w_o, q_gain[None], k_gain[None],
          jnp.asarray(cos), jnp.asarray(sin))
        return (y.reshape(hidden.shape), d_hidden.reshape(hidden.shape), d_wq, d_wk, d_wv, d_wo,
                small[0], small[1, :head_dim], small[1, head_dim:2 * head_dim])

    return jax.shard_map(local_step, mesh=mesh, in_specs=(seq_spec, replicated, replicated, replicated, replicated, replicated, replicated, replicated, seq_spec), out_specs=(seq_spec, seq_spec, replicated, replicated, replicated, replicated, replicated, replicated, replicated), check_vma=False)
```

```python
import math
import jax
import jax.numpy as jnp
import numpy as np
from jax import lax
from jax.experimental import pallas as pl
from jax.experimental.pallas import tpu as pltpu
from jax.sharding import PartitionSpec as P

ROPE_BASE = 1000000.0
NORM_EPS = 1e-6
LOG2E = 1.4426950408889634
F32 = jnp.float32
BF16 = jnp.bfloat16
QBLK = 256
VMEM_LIMIT = 35 * 1024 * 1024
COLOURS = ((1, 2, 3), (2, 3, 1), (3, 1, 2))
PER_POINT = 4
MASKS = (14, 12, 8, 6, 4, 10, 2, 15, 13, 9, 7, 5, 11, 3, 1)


def dot(a, b, ca, cb):
    return lax.dot_general(a, b, (((ca,), (cb,)), ((), ())), preferred_element_type=F32)


def rope_tables(n_pos, head_dim):
    half_dim = head_dim // 2
    inv_freq = np.exp(np.arange(half_dim, dtype=np.float32) * np.float32(-2.0 * math.log(ROPE_BASE) / head_dim))
    angles = np.arange(n_pos, dtype=np.float32)[:, None] * inv_freq[None, :]
    cos, sin = np.cos(angles), np.sin(angles)
    return np.concatenate([cos, cos], axis=-1), np.concatenate([-sin, sin], axis=-1)


def norm_rope(raw, gain, cos, sin):
    inv = lax.rsqrt(jnp.mean(raw * raw, axis=-1, keepdims=True) + NORM_EPS)
    unit = raw * inv
    normed = unit * gain
    return normed * cos + pltpu.roll(normed, raw.shape[-1] // 2, 1) * sin, unit, inv


def norm_rope_back(d_rot, unit, inv, gain, cos, sin):
    d_normed = d_rot * cos - pltpu.roll(d_rot, unit.shape[-1] // 2, 1) * sin
    d_gain = jnp.sum(d_normed * unit, axis=0, keepdims=True)
    d_unit = d_normed * gain
    return inv * (d_unit - unit * jnp.mean(d_unit * unit, axis=-1, keepdims=True)), d_gain


def causal_mask_t(scores_t, first_q):
    n_q = scores_t.shape[1]
    key = lax.broadcasted_iota(jnp.int32, (n_q, n_q), 0)
    query = lax.broadcasted_iota(jnp.int32, (n_q, n_q), 1)
    diag = jnp.where(query >= key, scores_t[first_q:], -1e30)
    if first_q == 0:
        return diag
    return jnp.concatenate([scores_t[:first_q], diag], axis=0)


def block_kernel(n_groups, *refs):
    n_steps = n_groups + 4

    def body(step, carry):
        block_step(step, n_steps, n_groups, *refs)
        return carry
    lax.fori_loop(0, n_steps, body, 0)


def block_step(step, n_steps, n_groups, hid_ref, dyin_ref, gain_ref, wq_ref, wk_ref, wv_ref, wo_ref, qg_ref, kg_ref,
               cos_ref, sin_ref, y_ref, dx_ref, u, small_ref,
               xs, dys, hs, ht, wcats, wos, dqkv, oall, y_acc, dn_acc, r0, r1, r2, r3, r4, sm, smr,
               in_send, in_recv, in_loc, d_send, d_recv, p_send, p_recv, g_send, g_recv, e_send, e_recv,
               s_send, s_recv, out_send, out_recv, out_loc, w_sem):
    n_dev, rows, n_loc, dim = hid_ref.shape
    n_pos = n_dev * n_loc
    head_dim = qg_ref.shape[-1]
    qw = wos.shape[1]
    group = qw // head_dim
    width = qw + 2 * head_dim
    half = u.shape[1] // 2
    lane = half // 2
    blk = lane // 3
    wcat, wo = wcats.at[step % 2], wos.at[step % 2]
    me = lax.axis_index('sp')
    bit = [(me // (1 << i)) % 2 for i in range(4)]
    partner = [me + (1 << i) * (1 - 2 * bit[i]) for i in range(4)]

    def remote(src, dst, send, recv, device):
        return pltpu.make_async_remote_copy(src_ref=src, dst_ref=dst, send_sem=send, recv_sem=recv,
                                            device_id=(device,), device_id_type=pl.DeviceIdType.MESH)

    def rows_of(g, start, size):
        return u.at[g, pl.ds(pl.multiple_of(start, 16), size)]

    own = [bit[0] * half + h * lane for h in range(2)]
    other = [(1 - bit[0]) * half + h * lane for h in range(2)]
    keep1, send1, keep2, send2, keep3, send3 = {}, {}, {}, {}, {}, {}
    for h in range(2):
        for c, (d1, d2, d3) in enumerate(COLOURS):
            base = own[h] + c * blk
            keep1[h, c] = base + bit[d1] * (blk // 2)
            send1[h, c] = base + (1 - bit[d1]) * (blk // 2)
            keep2[h, c] = keep1[h, c] + bit[d2] * (blk // 4)
            send2[h, c] = keep1[h, c] + (1 - bit[d2]) * (blk // 4)
            keep3[h, c] = keep2[h, c] + bit[d3] * (blk // 8)
            send3[h, c] = keep2[h, c] + (1 - bit[d3]) * (blk // 8)

    def core_scatter(g, h):
        return remote(rows_of(g, other[h], lane), r0.at[g % 2, h], d_send.at[h, g % 2], d_recv.at[h, g % 2], partner[0])

    def scatter(phase, c, g, h):
        start, size, buf = ((send1, blk // 2, r1), (send2, blk // 4, r2), (send3, blk // 8, r3))[phase]
        return remote(rows_of(g, start[h, c], size), buf.at[g % 2, h, c], p_send.at[phase, c, h, g % 2],
                      p_recv.at[phase, c, h, g % 2], partner[COLOURS[c][phase]])

    def gather(phase, c, g, h):
        start, size = ((keep3, blk // 8), (keep2, blk // 4), (keep1, blk // 2))[phase]
        part = rows_of(g, start[h, c], size)
        return remote(part, part if phase else r4.at[g % 2, h, c], g_send.at[phase, c, h, g % 2],
                      g_recv.at[phase, c, h, g % 2], partner[COLOURS[c][2 - phase]])

    def core_gather(g, h):
        part = rows_of(g, own[h], lane)
        return remote(part, part, e_send.at[h, g % 2], e_recv.at[h, g % 2], partner[0])

    def add_rows(g, start, size, buf):
        s = pl.ds(pl.multiple_of(start, 16), size)
        u[g, s] = u[g, s] + buf

    def stage(k, g, h):
        slot = g % 2
        if k == 1:
            core_scatter(g, h).wait()
            for c in range(3):
                add_rows(g, own[h] + c * blk, blk, r0[slot, h, c * blk:(c + 1) * blk])
                scatter(0, c, g, h).start()
        elif k in (2, 3, 4):
            keep, size, buf = ((keep1, blk // 2, r1), (keep2, blk // 4, r2), (keep3, blk // 8, r3))[k - 2]
            for c in range(3):
                scatter(k - 2, c, g, h).wait()
            for c in range(3):
                add_rows(g, keep[h, c], size, buf[slot, h, c])
                (scatter(k - 1, c, g, h) if k < 4 else gather(0, c, g, h)).start()
        elif k in (5, 6):
            for c in range(3):
                gather(k - 5, c, g, h).wait()
            for c in range(3):
                if k == 5:
                    u[g, pl.ds(pl.multiple_of(send3[h, c], 16), blk // 8)] = r4[slot, h, c]
                gather(k - 4, c, g, h).start()
        elif k == 7:
            for c in range(3):
                gather(2, c, g, h).wait()
            core_gather(g, h).start()
        else:
            core_gather(g, h).wait()

    sends = [(which, row, mask) for row in range(2) for which in (1, 0) for mask in MASKS]

    def handler(sub):
        h = sub % 2
        for k in range(8, 0, -1):
            if (2 * k - 2 + h - sub) % 4 == 0:
                g = step - 1 - (2 * k - 2 + h - sub) // 4

                @pl.when((g >= 0) & (g < n_groups))
                def _():
                    stage(k, g, h)
        for i in range(5):
            if (2 * i + 3) % 4 == sub:
                @pl.when(step == n_groups + (2 * i + 3) // 4)
                def _():
                    if i == 0:
                        small_copy(0).start()
                    else:
                        small_step(i - 1)
        for j in range(-(-len(sends) // PER_POINT)):
            if (j + 1) % 4 == sub:
                @pl.when(step == n_groups + (j + 1) // 4)
                def _():
                    for which, row, mask in sends[j * PER_POINT:(j + 1) * PER_POINT]:
                        to_peers(out_copy, which, row, (mask,))

    def small_copy(i):
        return remote(sm.at[i], smr.at[i], s_send.at[i], s_recv.at[i], partner[i])

    def small_step(i):
        small_copy(i).wait()
        sm[i + 1] = sm[i] + smr[i]
        if i < 3:
            small_copy(i + 1).start()
        else:
            small_ref[...] = sm[4]

    def in_copy(which, row, peer):
        src, dst = (hid_ref, xs) if which == 0 else (dyin_ref, dys)
        n = 2 * row + which
        return remote(src.at[peer, row], dst.at[row, me], in_send.at[n], in_recv.at[n], peer)

    def in_local(which, row):
        src, dst = (hid_ref, xs) if which == 0 else (dyin_ref, dys)
        return pltpu.make_async_copy(src.at[me, row], dst.at[row, me], in_loc.at[2 * row + which])

    def in_wait(which, row):
        dst = xs if which == 0 else dys
        n = 2 * row + which
        many = dst.at[row, pl.ds(0, n_dev - 1)]
        pltpu.make_async_copy(many, many, in_recv.at[n]).wait()
        in_local(which, row).wait()

    def in_wait_send(which, row):
        many = (xs if which == 0 else dys).at[row, pl.ds(0, n_dev - 1)]
        pltpu.make_async_copy(many, many, in_send.at[2 * row + which]).wait()

    def out_copy(which, row, peer):
        src, dst = (xs, y_ref) if which == 0 else (dys, dx_ref)
        n = 2 * row + which
        return remote(src.at[row, peer], dst.at[me, row], out_send.at[n], out_recv.at[n], peer)

    def out_local(which, row):
        src, dst = (xs, y_ref) if which == 0 else (dys, dx_ref)
        return pltpu.make_async_copy(src.at[row, me], dst.at[me, row], out_loc.at[2 * row + which])

    def to_peers(make, which, row, masks):
        for mask in masks:
            make(which, row, me + sum((mask & (1 << i)) * (1 - 2 * bit[i]) for i in range(4))).start()

    @pl.when(step == 0)
    def _():
        barrier = pltpu.get_barrier_semaphore()

        def greet(d, carry):
            pl.semaphore_signal(barrier, inc=1, device_id=(lax.rem(me + d, n_dev),), device_id_type=pl.DeviceIdType.MESH)
            return carry
        lax.fori_loop(1, n_dev, greet, 0)
        pl.semaphore_wait(barrier, n_dev - 1)
        for row in range(rows):
            for which in range(2):
                in_local(which, row).start()
                to_peers(in_copy, which, row, MASKS)
        y_acc[...] = jnp.zeros_like(y_acc)
        dn_acc[...] = jnp.zeros_like(dn_acc)
        sm[0] = jnp.zeros_like(sm[0])

    def tokens_of(row):
        return slice(row * n_pos, (row + 1) * n_pos)

    def row_compute(row):
        tok = tokens_of(row)
        cos, sin = cos_ref[...], sin_ref[...]
        scale = head_dim ** -0.5
        qkv = dot(hs[tok], wcat[...], 1, 0).astype(BF16)

        @pl.when(step == 0)
        def _():
            in_wait(1, row)
        d_o = dot(dys[row].reshape(n_pos, dim), wo[...], 1, 1).astype(BF16)
        k_rot, k_unit, k_inv = norm_rope(qkv[:, qw:qw + head_dim].astype(F32), kg_ref[...], cos, sin)
        k_rot = k_rot.astype(BF16)
        v = qkv[:, qw + head_dim:]
        dk_sum = [jnp.zeros((QBLK, head_dim), F32) for _ in range(n_pos // QBLK)]
        dv_sum = [jnp.zeros((QBLK, head_dim), F32) for _ in range(n_pos // QBLK)]
        for j in range(group):
            cols = slice(j * head_dim, (j + 1) * head_dim)
            q_rot, q_unit, q_inv = norm_rope(qkv[:, cols].astype(F32), qg_ref[...], cos, sin)
            q_rot = q_rot.astype(BF16)
            dq_parts = []
            for first in range(0, n_pos, QBLK):
                n_key = first + QBLK
                q_blk = q_rot[first:n_key]
                do_blk = d_o[first:n_key, cols]
                scores = causal_mask_t(dot(k_rot[:n_key], q_blk, 1, 1) * (scale * LOG2E), first)
                e = jnp.exp2(scores - jnp.max(scores, axis=0, keepdims=True))
                prob = e * (1.0 / jnp.sum(e, axis=0, keepdims=True))
                prob_bf = prob.astype(BF16)
                oall[row * n_pos + first:row * n_pos + n_key, cols] = dot(prob_bf, v[:n_key], 0, 0).astype(BF16)
                d_prob = dot(v[:n_key], do_blk, 1, 1)
                inner = jnp.sum(prob * d_prob, axis=0, keepdims=True)
                d_scores = (prob * (d_prob - inner) * scale).astype(BF16)
                dv_blk = dot(prob_bf, do_blk, 1, 0)
                dk_blk = dot(d_scores, q_blk, 1, 0)
                for i in range(n_key // QBLK):
                    dv_sum[i] += dv_blk[i * QBLK:(i + 1) * QBLK]
                    dk_sum[i] += dk_blk[i * QBLK:(i + 1) * QBLK]
                dq_parts.append(dot(d_scores, k_rot[:n_key], 0, 0))
            dq = jnp.concatenate(dq_parts, axis=0).astype(BF16).astype(F32)
            dq_raw, d_gain = norm_rope_back(dq, q_unit, q_inv, qg_ref[...], cos, sin)
            dqkv[tok, cols] = dq_raw.astype(BF16)
            sm[0, 1:2, :head_dim] += d_gain
        dk = jnp.concatenate(dk_sum, axis=0).astype(BF16).astype(F32)
        dk_raw, d_gain = norm_rope_back(dk, k_unit, k_inv, kg_ref[...], cos, sin)
        dqkv[tok, qw:qw + head_dim] = dk_raw.astype(BF16)
        sm[0, 1:2, head_dim:2 * head_dim] += d_gain
        dqkv[tok, qw + head_dim:] = jnp.concatenate(dv_sum, axis=0).astype(BF16)

    def input_norm(row):
        x = xs[row].reshape(n_pos, dim).astype(F32)
        inv = lax.rsqrt(jnp.mean(x * x, axis=-1, keepdims=True) + NORM_EPS)
        h = (x * inv * gain_ref[...]).astype(BF16)
        hs[tokens_of(row)] = h
        ht[:, tokens_of(row)] = h.T

    def finish_row(row):
        tok = tokens_of(row)
        x = xs[row].reshape(n_pos, dim).astype(F32)
        inv = lax.rsqrt(jnp.mean(x * x, axis=-1, keepdims=True) + NORM_EPS)
        unit = x * inv
        d_normed = dn_acc[tok]
        sm[0, 0:1] += jnp.sum(d_normed * unit, axis=0, keepdims=True)
        d_unit = d_normed * gain_ref[...]
        d_x = inv * (d_unit - unit * jnp.mean(d_unit * unit, axis=-1, keepdims=True))
        d_y = dys[row].reshape(n_pos, dim).astype(F32)
        dys[row] = (d_y + d_x).astype(BF16).reshape(n_dev, n_loc, dim)
        xs[row] = (x + y_acc[tok]).astype(BF16).reshape(n_dev, n_loc, dim)

    computing = step < n_groups

    def weight_copies(g):
        slot = g % 2
        col = lambda n: pl.ds(pl.multiple_of(g * n, 128), n)
        pieces = ((wq_ref.at[:, col(qw)], wcats.at[slot, :, :qw]),
                  (wk_ref.at[:, col(head_dim)], wcats.at[slot, :, qw:qw + head_dim]),
                  (wv_ref.at[:, col(head_dim)], wcats.at[slot, :, qw + head_dim:]),
                  (wo_ref.at[col(qw)], wos.at[slot]))
        return [pltpu.make_async_copy(a, b, w_sem.at[slot, i]) for i, (a, b) in enumerate(pieces)]

    @pl.when(computing)
    def _():
        @pl.when(step == 0)
        def _():
            for copy in weight_copies(0):
                copy.start()
        for copy in weight_copies(step):
            copy.wait()

        @pl.when(step + 1 < n_groups)
        def _():
            for copy in weight_copies(step + 1):
                copy.start()

    for row in range(rows):
        handler(row)

        @pl.when(step == 0)
        def _():
            in_wait(0, row)
            input_norm(row)

        @pl.when(computing)
        def _():
            row_compute(row)

        @pl.when(step == n_groups)
        def _():
            for which in range(2):
                in_wait_send(which, row)
            finish_row(row)
            for which in range(2):
                out_local(which, row).start()

    handler(2)

    @pl.when(computing)
    def _():
        u[step, :dim] = dot(ht[...], dqkv[...], 1, 0)
        d_wo = dot(oall[...], dys[...].reshape(rows * n_pos, dim), 0, 0)
        u[step, dim:dim + qw] = d_wo[:, :width]
        u[step, dim + qw:] = d_wo[:, width:]
        for h in range(2):
            core_scatter(step, h).start()

    handler(3)

    @pl.when(computing)
    def _():
        y_acc[...] += dot(oall[...], wo[...], 1, 0)
        dn_acc[...] += dot(dqkv[...], wcat[...], 1, 1)

    @pl.when(step == n_steps - 1)
    def _():
        for row in range(rows):
            for which in range(2):
                n = 2 * row + which
                many = (xs if which == 0 else dys).at[row, pl.ds(0, n_dev - 1)]
                landed = (y_ref if which == 0 else dx_ref).at[pl.ds(0, n_dev - 1), row]
                pltpu.make_async_copy(many, many, out_send.at[n]).wait()
                pltpu.make_async_copy(landed, landed, out_recv.at[n]).wait()
                out_local(which, row).wait()


def place_kernel(y_in, dx_in, u, small, y_ref, dx_ref, dwq_ref, dwk_ref, dwv_ref, dwo_ref, dg_ref, dqg_ref, dkg_ref,
                 out_sem, w_sem, s_sem):
    dim, head_dim = dg_ref.shape[1], dqg_ref.shape[1]
    n_groups, _, width = u.shape
    qw = dwq_ref.shape[1] // n_groups
    stores = []
    for g in range(n_groups):
        col = lambda n: slice(g * n, (g + 1) * n)
        pieces = ((u.at[g, :dim, :qw], dwq_ref.at[:, col(qw)]),
                  (u.at[g, :dim, qw:qw + head_dim], dwk_ref.at[:, col(head_dim)]),
                  (u.at[g, :dim, qw + head_dim:], dwv_ref.at[:, col(head_dim)]),
                  (u.at[g, dim:dim + qw], dwo_ref.at[col(qw), :width]),
                  (u.at[g, dim + qw:], dwo_ref.at[col(qw), width:]))
        stores += [pltpu.make_async_copy(src, dst, w_sem.at[g, i]) for i, (src, dst) in enumerate(pieces)]
    stores += [pltpu.make_async_copy(src, dst, s_sem.at[i]) for i, (src, dst) in enumerate((
        (small.at[0:1], dg_ref), (small.at[1:2, :head_dim], dqg_ref), (small.at[1:2, head_dim:2 * head_dim], dkg_ref)))]
    stores += [pltpu.make_async_copy(src, dst, out_sem.at[i]) for i, (src, dst) in enumerate(((y_in, y_ref), (dx_in, dx_ref)))]
    for copy in stores:
        copy.start()
    for copy in stores:
        copy.wait()


def solution(mesh):
    n_dev = mesh.shape['sp']
    seq_spec = P(None, 'sp', None)
    replicated = P()

    def local_step(hidden, norm_gain, w_q, w_k, w_v, q_gain, k_gain, w_o, d_out):
        n_batch, n_loc, dim = hidden.shape
        head_dim = q_gain.shape[0]
        kv_heads = w_k.shape[1] // head_dim
        qw = w_q.shape[1] // kv_heads
        width = qw + 2 * head_dim
        rows = n_batch // n_dev
        n_pos = n_loc * n_dev
        tokens = rows * n_pos
        cos, sin = rope_tables(n_pos, head_dim)
        slice_rows = dim + 2 * qw
        lane = slice_rows // 4
        blk = lane // 3
        anywhere = pl.BlockSpec(memory_space=pl.ANY)
        in_vmem = pl.BlockSpec(memory_space=pltpu.VMEM)
        act = (n_dev, rows, n_loc, dim)
        dma = pltpu.SemaphoreType.DMA
        y, d_hidden, slices, small = pl.pallas_call(
            lambda *refs: block_kernel(kv_heads, *refs),
            in_specs=[anywhere, anywhere, in_vmem, anywhere, anywhere, anywhere, anywhere] + [in_vmem] * 4,
            out_specs=[in_vmem] * 4,
            out_shape=[
                pltpu.VMEM(act, BF16), pltpu.VMEM(act, BF16),
                pltpu.VMEM((kv_heads, slice_rows, width), F32), pltpu.VMEM((8, dim), F32)],
            scratch_shapes=[
                pltpu.VMEM((rows, n_dev, n_loc, dim), BF16), pltpu.VMEM((rows, n_dev, n_loc, dim), BF16),
                pltpu.VMEM((tokens, dim), BF16), pltpu.VMEM((dim, tokens), BF16),
                pltpu.VMEM((2, dim, width), BF16), pltpu.VMEM((2, qw, dim), BF16),
                pltpu.VMEM((tokens, width), BF16), pltpu.VMEM((tokens, qw), BF16),
                pltpu.VMEM((tokens, dim), F32), pltpu.VMEM((tokens, dim), F32),
                pltpu.VMEM((2, 2, lane, width), F32), pltpu.VMEM((2, 2, 3, blk // 2, width), F32),
                pltpu.VMEM((2, 2, 3, blk // 4, width), F32), pltpu.VMEM((2, 2, 3, blk // 8, width), F32),
                pltpu.VMEM((2, 2, 3, blk // 8, width), F32),
                pltpu.VMEM((5, 8, dim), F32), pltpu.VMEM((4, 8, dim), F32),
                dma((4,)), dma((4,)), dma((4,)), dma((2, 2)), dma((2, 2)), dma((3, 3, 2, 2)), dma((3, 3, 2, 2)),
                dma((3, 3, 2, 2)), dma((3, 3, 2, 2)), dma((2, 2)), dma((2, 2)), dma((4,)), dma((4,)),
                dma((4,)), dma((4,)), dma((4,)), dma((2, 4))],
            compiler_params=pltpu.CompilerParams(
                vmem_limit_bytes=VMEM_LIMIT, collective_id=0, has_side_effects=True),
            cost_estimate=pl.CostEstimate(flops=52 * 10**9, bytes_accessed=50 * 10**6, transcendentals=0),
            name='attn_block',
        )(hidden.reshape(act), d_out.reshape(act), norm_gain[None], w_q, w_k, w_v, w_o, q_gain[None], k_gain[None],
          jnp.asarray(cos), jnp.asarray(sin))
        y, d_hidden, d_wq, d_wk, d_wv, d_wo, d_ng, d_qg, d_kg = pl.pallas_call(
            place_kernel,
            in_specs=[in_vmem] * 4,
            out_specs=[anywhere] * 9,
            out_shape=[
                jax.ShapeDtypeStruct(act, BF16), jax.ShapeDtypeStruct(act, BF16),
                jax.ShapeDtypeStruct(w_q.shape, F32), jax.ShapeDtypeStruct(w_k.shape, F32),
                jax.ShapeDtypeStruct(w_v.shape, F32), jax.ShapeDtypeStruct(w_o.shape, F32),
                jax.ShapeDtypeStruct((1, dim), F32), jax.ShapeDtypeStruct((1, head_dim), F32),
                jax.ShapeDtypeStruct((1, head_dim), F32)],
            scratch_shapes=[dma((2,)), dma((kv_heads, 5)), dma((3,))],
            compiler_params=pltpu.CompilerParams(vmem_limit_bytes=4 * 1024 * 1024),
            cost_estimate=pl.CostEstimate(flops=10**9, bytes_accessed=60 * 10**6, transcendentals=0),
            name='pack_out',
        )(*[pltpu.with_memory_space_constraint(a, pltpu.VMEM) for a in (y, d_hidden, slices, small)])
        return (y.reshape(hidden.shape), d_hidden.reshape(hidden.shape), d_wq, d_wk, d_wv, d_wo, d_ng[0], d_qg[0], d_kg[0])

    return jax.shard_map(local_step, mesh=mesh, in_specs=(seq_spec, replicated, replicated, replicated, replicated, replicated, replicated, replicated, seq_spec), out_specs=(seq_spec, seq_spec, replicated, replicated, replicated, replicated, replicated, replicated, replicated), check_vma=False)
```

```python
import math
import jax
import jax.numpy as jnp
import numpy as np
from jax import lax
from jax.experimental import pallas as pl
from jax.experimental.pallas import tpu as pltpu
from jax.sharding import PartitionSpec as P

ROPE_BASE = 1000000.0
NORM_EPS = 1e-6
LOG2E = 1.4426950408889634
F32 = jnp.float32
BF16 = jnp.bfloat16
QBLK = 256
OUT_MASKS = (14, 12, 8, 6, 4, 10, 2, 15, 13, 9, 7, 5, 11, 3, 1)
AHEAD = 3
VMEM_LIMIT = 36640 * 1024
COLOURS = ((1, 2, 3), (2, 3, 1), (3, 1, 2))
PER_POINT = 4
MASKS = (8, 4, 2, 12, 10, 6, 14, 9, 5, 3, 13, 11, 7, 15, 1)


def dot(a, b, ca, cb):
    return lax.dot_general(a, b, (((ca,), (cb,)), ((), ())), preferred_element_type=F32)


def rope_tables(n_pos, head_dim):
    half_dim = head_dim // 2
    inv_freq = np.exp(np.arange(half_dim, dtype=np.float32) * np.float32(-2.0 * math.log(ROPE_BASE) / head_dim))
    angles = np.arange(n_pos, dtype=np.float32)[:, None] * inv_freq[None, :]
    cos, sin = np.cos(angles), np.sin(angles)
    return np.concatenate([cos, cos], axis=-1), np.concatenate([-sin, sin], axis=-1)


def norm_rope(raw, gain, cos, sin):
    inv = lax.rsqrt(jnp.mean(raw * raw, axis=-1, keepdims=True) + NORM_EPS)
    unit = raw * inv
    normed = unit * gain
    return normed * cos + pltpu.roll(normed, raw.shape[-1] // 2, 1) * sin, unit, inv


def norm_rope_back(d_rot, unit, inv, gain, cos, sin):
    d_normed = d_rot * cos - pltpu.roll(d_rot, unit.shape[-1] // 2, 1) * sin
    d_gain = jnp.sum(d_normed * unit, axis=0, keepdims=True)
    d_unit = d_normed * gain
    return inv * (d_unit - unit * jnp.mean(d_unit * unit, axis=-1, keepdims=True)), d_gain


def causal_mask_t(scores_t, first_q):
    n_q = scores_t.shape[1]
    key = lax.broadcasted_iota(jnp.int32, (n_q, n_q), 0)
    query = lax.broadcasted_iota(jnp.int32, (n_q, n_q), 1)
    diag = jnp.where(query >= key, scores_t[first_q:], -1e30)
    if first_q == 0:
        return diag
    return jnp.concatenate([scores_t[:first_q], diag], axis=0)


def block_kernel(n_groups, *refs):
    n_steps = n_groups + 4

    def body(step, carry):
        block_step(step, n_steps, n_groups, *refs)
        return carry
    lax.fori_loop(0, n_steps, body, 0)


def block_step(step, n_steps, n_groups, hid_ref, dyin_ref, gain_ref, wq_ref, wk_ref, wv_ref, wo_ref, qg_ref, kg_ref,
               cos_ref, sin_ref, y_ref, dx_ref, u, small_ref,
               xs, dys, hs, ht, wcats, wos, dqkv, oall, dqkv_early, o_early, y_acc, dn_acc, r0, r1, r2, r3, r4, sm, smr,
               in_send, in_recv, in_loc, d_send, d_recv, p_send, p_recv, g_send, g_recv, e_send, e_recv,
               s_send, s_recv, out_send, out_recv, out_loc, w_sem):
    n_dev, rows, n_loc, dim = hid_ref.shape
    n_pos = n_dev * n_loc
    head_dim = qg_ref.shape[-1]
    qw = wos.shape[1]
    group = qw // head_dim
    width = qw + 2 * head_dim
    half = u.shape[1] // 2
    lane = half // 2
    blk = lane // 3
    me = lax.axis_index('sp')
    bit = [(me // (1 << i)) % 2 for i in range(4)]
    partner = [me + (1 << i) * (1 - 2 * bit[i]) for i in range(4)]

    def remote(src, dst, send, recv, device):
        return pltpu.make_async_remote_copy(src_ref=src, dst_ref=dst, send_sem=send, recv_sem=recv,
                                            device_id=(device,), device_id_type=pl.DeviceIdType.MESH)

    def rows_of(g, start, size):
        return u.at[g, pl.ds(pl.multiple_of(start, 16), size)]

    own = [bit[0] * half + h * lane for h in range(2)]
    other = [(1 - bit[0]) * half + h * lane for h in range(2)]
    keep1, send1, keep2, send2, keep3, send3 = {}, {}, {}, {}, {}, {}
    for h in range(2):
        for c, (d1, d2, d3) in enumerate(COLOURS):
            base = own[h] + c * blk
            keep1[h, c] = base + bit[d1] * (blk // 2)
            send1[h, c] = base + (1 - bit[d1]) * (blk // 2)
            keep2[h, c] = keep1[h, c] + bit[d2] * (blk // 4)
            send2[h, c] = keep1[h, c] + (1 - bit[d2]) * (blk // 4)
            keep3[h, c] = keep2[h, c] + bit[d3] * (blk // 8)
            send3[h, c] = keep2[h, c] + (1 - bit[d3]) * (blk // 8)

    def core_scatter(g, h):
        return remote(rows_of(g, other[h], lane), r0.at[g % 2, h], d_send.at[h, g % 2], d_recv.at[h, g % 2], partner[0])

    def scatter(phase, c, g, h):
        start, size, buf = ((send1, blk // 2, r1), (send2, blk // 4, r2), (send3, blk // 8, r3))[phase]
        return remote(rows_of(g, start[h, c], size), buf.at[g % 2, h, c], p_send.at[phase, c, h, g % 2],
                      p_recv.at[phase, c, h, g % 2], partner[COLOURS[c][phase]])

    def gather(phase, c, g, h):
        start, size = ((keep3, blk // 8), (keep2, blk // 4), (keep1, blk // 2))[phase]
        part = rows_of(g, start[h, c], size)
        return remote(part, part if phase else r4.at[g % 2, h, c], g_send.at[phase, c, h, g % 2],
                      g_recv.at[phase, c, h, g % 2], partner[COLOURS[c][2 - phase]])

    def core_gather(g, h):
        part = rows_of(g, own[h], lane)
        return remote(part, part, e_send.at[h, g % 2], e_recv.at[h, g % 2], partner[0])

    def add_rows(g, start, size, buf):
        s = pl.ds(pl.multiple_of(start, 16), size)
        u[g, s] = u[g, s] + buf

    def stage(k, g, h):
        slot = g % 2
        if k == 1:
            core_scatter(g, h).wait()
            for c in range(3):
                add_rows(g, own[h] + c * blk, blk, r0[slot, h, c * blk:(c + 1) * blk])
                scatter(0, c, g, h).start()
        elif k in (2, 3, 4):
            keep, size, buf = ((keep1, blk // 2, r1), (keep2, blk // 4, r2), (keep3, blk // 8, r3))[k - 2]
            for c in range(3):
                scatter(k - 2, c, g, h).wait()
            for c in range(3):
                add_rows(g, keep[h, c], size, buf[slot, h, c])
                (scatter(k - 1, c, g, h) if k < 4 else gather(0, c, g, h)).start()
        elif k in (5, 6):
            for c in range(3):
                gather(k - 5, c, g, h).wait()
            for c in range(3):
                if k == 5:
                    u[g, pl.ds(pl.multiple_of(send3[h, c], 16), blk // 8)] = r4[slot, h, c]
                gather(k - 4, c, g, h).start()
        elif k == 7:
            for c in range(3):
                gather(2, c, g, h).wait()
            core_gather(g, h).start()
        else:
            core_gather(g, h).wait()

    sends = [(which, row, mask) for row in range(2) for which in (1, 0) for mask in OUT_MASKS]

    def handler(sub):
        h = sub % 2
        for k in range(8, 0, -1):
            if (2 * k - 2 + h - sub) % 4 == 0:
                g = step - 1 - (2 * k - 2 + h - sub) // 4

                @pl.when((g >= 0) & (g < n_groups))
                def _():
                    stage(k, g, h)
        for i in range(5):
            if (2 * i + 3) % 4 == sub:
                @pl.when(step == n_groups + (2 * i + 3) // 4)
                def _():
                    if i == 0:
                        small_copy(0).start()
                    else:
                        small_step(i - 1)
        for j in range(-(-len(sends) // PER_POINT)):
            if (j + 1) % 4 == sub:
                @pl.when(step == n_groups + (j + 1) // 4)
                def _():
                    for which, row, mask in sends[j * PER_POINT:(j + 1) * PER_POINT]:
                        to_peers(out_copy, which, row, (mask,))

    def small_copy(i):
        return remote(sm.at[i], smr.at[i], s_send.at[i], s_recv.at[i], partner[i])

    def small_step(i):
        small_copy(i).wait()
        sm[i + 1] = sm[i] + smr[i]
        if i < 3:
            small_copy(i + 1).start()
        else:
            small_ref[...] = sm[4]

    def in_copy(which, row, peer):
        src, dst = (hid_ref, xs) if which == 0 else (dyin_ref, dys)
        n = 2 * row + which
        return remote(src.at[peer, row], dst.at[row, me], in_send.at[n], in_recv.at[n], peer)

    def in_local(which, row):
        src, dst = (hid_ref, xs) if which == 0 else (dyin_ref, dys)
        return pltpu.make_async_copy(src.at[me, row], dst.at[row, me], in_loc.at[2 * row + which])

    def in_wait(which, row):
        dst = xs if which == 0 else dys
        n = 2 * row + which
        many = dst.at[row, pl.ds(0, n_dev - 1)]
        pltpu.make_async_copy(many, many, in_recv.at[n]).wait()
        in_local(which, row).wait()

    def in_wait_send(which, row):
        many = (xs if which == 0 else dys).at[row, pl.ds(0, n_dev - 1)]
        pltpu.make_async_copy(many, many, in_send.at[2 * row + which]).wait()

    def out_copy(which, row, peer):
        src, dst = (xs, y_ref) if which == 0 else (dys, dx_ref)
        n = 2 * row + which
        return remote(src.at[row, peer], dst.at[me, row], out_send.at[n], out_recv.at[n], peer)

    def out_local(which, row):
        src, dst = (xs, y_ref) if which == 0 else (dys, dx_ref)
        return pltpu.make_async_copy(src.at[row, me], dst.at[me, row], out_loc.at[2 * row + which])

    def to_peers(make, which, row, masks):
        for mask in masks:
            make(which, row, me + sum((mask & (1 << i)) * (1 - 2 * bit[i]) for i in range(4))).start()

    @pl.when(step == 0)
    def _():
        barrier = pltpu.get_barrier_semaphore()

        def greet(d, carry):
            pl.semaphore_signal(barrier, inc=1, device_id=(lax.rem(me + d, n_dev),), device_id_type=pl.DeviceIdType.MESH)
            return carry
        lax.fori_loop(1, n_dev, greet, 0)
        pl.semaphore_wait(barrier, n_dev - 1)
        for row in range(rows):
            for which in range(2):
                in_local(which, row).start()
                to_peers(in_copy, which, row, MASKS)
        y_acc[...] = jnp.zeros_like(y_acc)
        dn_acc[...] = jnp.zeros_like(dn_acc)
        sm[0] = jnp.zeros_like(sm[0])

    def tokens_of(row):
        return slice(row * n_pos, (row + 1) * n_pos)

    def row_compute(row, g, arriving, d_to, o_to):
        tok = tokens_of(row)
        wcat, wo = wcats.at[g % 2], wos.at[g % 2]
        cos, sin = cos_ref[...], sin_ref[...]
        scale = head_dim ** -0.5
        qkv = dot(hs[tok], wcat[...], 1, 0).astype(BF16)

        def grad_heads():
            return dot(dys[row].reshape(n_pos, dim), wo[...], 1, 1).astype(BF16)

        def probs_of(first, q_blk, cols):
            n_key = first + QBLK
            scores = causal_mask_t(dot(k_rot[:n_key], q_blk, 1, 1) * (scale * LOG2E), first)
            e = jnp.exp2(scores - jnp.max(scores, axis=0, keepdims=True))
            prob = e * (1.0 / jnp.sum(e, axis=0, keepdims=True))
            prob_bf = prob.astype(BF16)
            o_to[first:n_key, cols] = dot(prob_bf, v[:n_key], 0, 0).astype(BF16)
            return prob, prob_bf

        k_rot, k_unit, k_inv = norm_rope(qkv[:, qw:qw + head_dim].astype(F32), kg_ref[...], cos, sin)
        k_rot = k_rot.astype(BF16)
        v = qkv[:, qw + head_dim:]
        if arriving:
            early = []
            for j in range(group):
                cols = slice(j * head_dim, (j + 1) * head_dim)
                q_rot, q_unit, q_inv = norm_rope(qkv[:, cols].astype(F32), qg_ref[...], cos, sin)
                q_rot = q_rot.astype(BF16)
                early.append((q_rot, q_unit, q_inv, [probs_of(first, q_rot[first:first + QBLK], cols) for first in range(0, n_pos, QBLK)]))
            in_wait(1, row)
        d_o = grad_heads()
        dk_sum = [jnp.zeros((QBLK, head_dim), F32) for _ in range(n_pos // QBLK)]
        dv_sum = [jnp.zeros((QBLK, head_dim), F32) for _ in range(n_pos // QBLK)]
        for j in range(group):
            cols = slice(j * head_dim, (j + 1) * head_dim)
            if arriving:
                q_rot, q_unit, q_inv, probs = early[j]
            else:
                q_rot, q_unit, q_inv = norm_rope(qkv[:, cols].astype(F32), qg_ref[...], cos, sin)
                q_rot = q_rot.astype(BF16)
            dq_parts = []
            for first in range(0, n_pos, QBLK):
                n_key = first + QBLK
                q_blk = q_rot[first:n_key]
                do_blk = d_o[first:n_key, cols]
                prob, prob_bf = probs[first // QBLK] if arriving else probs_of(first, q_blk, cols)
                d_prob = dot(v[:n_key], do_blk, 1, 1)
                inner = jnp.sum(prob * d_prob, axis=0, keepdims=True)
                d_scores = (prob * (d_prob - inner)).astype(BF16)
                dv_blk = dot(prob_bf, do_blk, 1, 0)
                dk_blk = dot(d_scores, q_blk, 1, 0)
                for i in range(n_key // QBLK):
                    dv_sum[i] += dv_blk[i * QBLK:(i + 1) * QBLK]
                    dk_sum[i] += dk_blk[i * QBLK:(i + 1) * QBLK]
                dq_parts.append(dot(d_scores, k_rot[:n_key], 0, 0))
            dq = (jnp.concatenate(dq_parts, axis=0) * scale).astype(BF16).astype(F32)
            dq_raw, d_gain = norm_rope_back(dq, q_unit, q_inv, qg_ref[...], cos, sin)
            d_to[:, cols] = dq_raw.astype(BF16)
            sm[0, 1:2, :head_dim] += d_gain
        dk = (jnp.concatenate(dk_sum, axis=0) * scale).astype(BF16).astype(F32)
        dk_raw, d_gain = norm_rope_back(dk, k_unit, k_inv, kg_ref[...], cos, sin)
        d_to[:, qw:qw + head_dim] = dk_raw.astype(BF16)
        sm[0, 1:2, head_dim:2 * head_dim] += d_gain
        d_to[:, qw + head_dim:] = jnp.concatenate(dv_sum, axis=0).astype(BF16)

    def input_norm(row):
        x = xs[row].reshape(n_pos, dim).astype(F32)
        inv = lax.rsqrt(jnp.mean(x * x, axis=-1, keepdims=True) + NORM_EPS)
        h = (x * inv * gain_ref[...]).astype(BF16)
        hs[tokens_of(row)] = h
        ht[:, tokens_of(row)] = h.T

    def finish_row(row):
        tok = tokens_of(row)
        x = xs[row].reshape(n_pos, dim).astype(F32)
        inv = lax.rsqrt(jnp.mean(x * x, axis=-1, keepdims=True) + NORM_EPS)
        unit = x * inv
        d_normed = dn_acc[tok]
        sm[0, 0:1] += jnp.sum(d_normed * unit, axis=0, keepdims=True)
        d_unit = d_normed * gain_ref[...]
        d_x = inv * (d_unit - unit * jnp.mean(d_unit * unit, axis=-1, keepdims=True))
        d_y = dys[row].reshape(n_pos, dim).astype(F32)
        dys[row] = (d_y + d_x).astype(BF16).reshape(n_dev, n_loc, dim)
        xs[row] = (x + y_acc[tok]).astype(BF16).reshape(n_dev, n_loc, dim)

    computing = step < n_groups

    def weight_copies(g):
        slot = g % 2
        col = lambda n: pl.ds(pl.multiple_of(g * n, 128), n)
        pieces = ((wq_ref.at[:, col(qw)], wcats.at[slot, :, :qw]),
                  (wk_ref.at[:, col(head_dim)], wcats.at[slot, :, qw:qw + head_dim]),
                  (wv_ref.at[:, col(head_dim)], wcats.at[slot, :, qw + head_dim:]),
                  (wo_ref.at[col(qw)], wos.at[slot]))
        return [pltpu.make_async_copy(a, b, w_sem.at[slot, i]) for i, (a, b) in enumerate(pieces)]

    def weights(g, n):
        for copy in weight_copies(g):
            copy.wait()

        @pl.when(g + 1 < n)
        def _():
            for copy in weight_copies(g + 1):
                copy.start()

    @pl.when(step == 0)
    def _():
        for copy in weight_copies(0):
            copy.start()
        in_wait(0, 0)
        input_norm(0)
        in_wait(1, 0)

        def first_row(g, carry):
            weights(g, AHEAD)
            row_compute(0, g, False, dqkv_early.at[g], o_early.at[g])
            return carry
        lax.fori_loop(0, AHEAD, first_row, 0)
        for copy in weight_copies(0):
            copy.start()
        in_wait(0, 1)
        input_norm(1)

    @pl.when(computing)
    def _():
        weights(step, n_groups)

    for row in range(rows):
        handler(row)

        if row == 0:
            @pl.when(step < AHEAD)
            def _():
                dqkv[:n_pos] = dqkv_early[step]
                oall[:n_pos] = o_early[step]

        def into(row, arriving):
            row_compute(row, step, arriving, dqkv.at[tokens_of(row)], oall.at[tokens_of(row)])

        if row == 1:
            @pl.when(step == 0)
            def _():
                into(row, True)

        @pl.when(computing & (step >= (AHEAD if row == 0 else 1)))
        def _():
            into(row, False)

        @pl.when(step == n_groups)
        def _():
            for which in range(2):
                in_wait_send(which, row)
            finish_row(row)
            for which in range(2):
                out_local(which, row).start()

    handler(2)

    @pl.when(computing)
    def _():
        u[step, :dim] = dot(ht[...], dqkv[...], 1, 0)
        d_wo = dot(oall[...], dys[...].reshape(rows * n_pos, dim), 0, 0)
        u[step, dim:dim + qw] = d_wo[:, :width]
        u[step, dim + qw:] = d_wo[:, width:]
        for h in range(2):
            core_scatter(step, h).start()

    handler(3)

    @pl.when(computing)
    def _():
        y_acc[...] += dot(oall[...], wos[step % 2], 1, 0)
        dn_acc[...] += dot(dqkv[...], wcats[step % 2], 1, 1)

    @pl.when(step == n_steps - 1)
    def _():
        for row in range(rows):
            for which in range(2):
                n = 2 * row + which
                many = (xs if which == 0 else dys).at[row, pl.ds(0, n_dev - 1)]
                landed = (y_ref if which == 0 else dx_ref).at[pl.ds(0, n_dev - 1), row]
                pltpu.make_async_copy(many, many, out_send.at[n]).wait()
                pltpu.make_async_copy(landed, landed, out_recv.at[n]).wait()
                out_local(which, row).wait()


def place_kernel(y_in, dx_in, u, small, y_ref, dx_ref, dwq_ref, dwk_ref, dwv_ref, dwo_ref, dg_ref, dqg_ref, dkg_ref,
                 out_sem, w_sem, s_sem):
    dim, head_dim = dg_ref.shape[1], dqg_ref.shape[1]
    n_groups, _, width = u.shape
    qw = dwq_ref.shape[1] // n_groups
    stores = []
    for g in range(n_groups):
        col = lambda n: slice(g * n, (g + 1) * n)
        pieces = ((u.at[g, :dim, :qw], dwq_ref.at[:, col(qw)]),
                  (u.at[g, :dim, qw:qw + head_dim], dwk_ref.at[:, col(head_dim)]),
                  (u.at[g, :dim, qw + head_dim:], dwv_ref.at[:, col(head_dim)]),
                  (u.at[g, dim:dim + qw], dwo_ref.at[col(qw), :width]),
                  (u.at[g, dim + qw:], dwo_ref.at[col(qw), width:]))
        stores += [pltpu.make_async_copy(src, dst, w_sem.at[g, i]) for i, (src, dst) in enumerate(pieces)]
    stores += [pltpu.make_async_copy(src, dst, s_sem.at[i]) for i, (src, dst) in enumerate((
        (small.at[0:1], dg_ref), (small.at[1:2, :head_dim], dqg_ref), (small.at[1:2, head_dim:2 * head_dim], dkg_ref)))]
    stores += [pltpu.make_async_copy(src, dst, out_sem.at[i]) for i, (src, dst) in enumerate(((y_in, y_ref), (dx_in, dx_ref)))]
    for copy in stores:
        copy.start()
    for copy in stores:
        copy.wait()


def solution(mesh):
    n_dev = mesh.shape['sp']
    seq_spec = P(None, 'sp', None)
    replicated = P()

    def local_step(hidden, norm_gain, w_q, w_k, w_v, q_gain, k_gain, w_o, d_out):
        n_batch, n_loc, dim = hidden.shape
        head_dim = q_gain.shape[0]
        kv_heads = w_k.shape[1] // head_dim
        qw = w_q.shape[1] // kv_heads
        width = qw + 2 * head_dim
        rows = n_batch // n_dev
        n_pos = n_loc * n_dev
        tokens = rows * n_pos
        cos, sin = rope_tables(n_pos, head_dim)
        slice_rows = dim + 2 * qw
        lane = slice_rows // 4
        blk = lane // 3
        anywhere = pl.BlockSpec(memory_space=pl.ANY)
        in_vmem = pl.BlockSpec(memory_space=pltpu.VMEM)
        act = (n_dev, rows, n_loc, dim)
        dma = pltpu.SemaphoreType.DMA
        y, d_hidden, slices, small = pl.pallas_call(
            lambda *refs: block_kernel(kv_heads, *refs),
            in_specs=[anywhere, anywhere, in_vmem, anywhere, anywhere, anywhere, anywhere] + [in_vmem] * 4,
            out_specs=[in_vmem] * 4,
            out_shape=[
                pltpu.VMEM(act, BF16), pltpu.VMEM(act, BF16),
                pltpu.VMEM((kv_heads, slice_rows, width), F32), pltpu.VMEM((8, dim), F32)],
            scratch_shapes=[
                pltpu.VMEM((rows, n_dev, n_loc, dim), BF16), pltpu.VMEM((rows, n_dev, n_loc, dim), BF16),
                pltpu.VMEM((tokens, dim), BF16), pltpu.VMEM((dim, tokens), BF16),
                pltpu.VMEM((2, dim, width), BF16), pltpu.VMEM((2, qw, dim), BF16),
                pltpu.VMEM((tokens, width), BF16), pltpu.VMEM((tokens, qw), BF16),
                pltpu.VMEM((AHEAD, n_pos, width), BF16), pltpu.VMEM((AHEAD, n_pos, qw), BF16),
                pltpu.VMEM((tokens, dim), F32), pltpu.VMEM((tokens, dim), F32),
                pltpu.VMEM((2, 2, lane, width), F32), pltpu.VMEM((2, 2, 3, blk // 2, width), F32),
                pltpu.VMEM((2, 2, 3, blk // 4, width), F32), pltpu.VMEM((2, 2, 3, blk // 8, width), F32),
                pltpu.VMEM((2, 2, 3, blk // 8, width), F32),
                pltpu.VMEM((5, 8, dim), F32), pltpu.VMEM((4, 8, dim), F32),
                dma((4,)), dma((4,)), dma((4,)), dma((2, 2)), dma((2, 2)), dma((3, 3, 2, 2)), dma((3, 3, 2, 2)),
                dma((3, 3, 2, 2)), dma((3, 3, 2, 2)), dma((2, 2)), dma((2, 2)), dma((4,)), dma((4,)),
                dma((4,)), dma((4,)), dma((4,)), dma((2, 4))],
            compiler_params=pltpu.CompilerParams(
                vmem_limit_bytes=VMEM_LIMIT, collective_id=0, has_side_effects=True),
            cost_estimate=pl.CostEstimate(flops=52 * 10**9, bytes_accessed=50 * 10**6, transcendentals=0),
            name='attn_block',
        )(hidden.reshape(act), d_out.reshape(act), norm_gain[None], w_q, w_k, w_v, w_o, q_gain[None], k_gain[None],
          jnp.asarray(cos), jnp.asarray(sin))
        y, d_hidden, d_wq, d_wk, d_wv, d_wo, d_ng, d_qg, d_kg = pl.pallas_call(
            place_kernel,
            in_specs=[in_vmem] * 4,
            out_specs=[anywhere] * 9,
            out_shape=[
                jax.ShapeDtypeStruct(act, BF16), jax.ShapeDtypeStruct(act, BF16),
                jax.ShapeDtypeStruct(w_q.shape, F32), jax.ShapeDtypeStruct(w_k.shape, F32),
                jax.ShapeDtypeStruct(w_v.shape, F32), jax.ShapeDtypeStruct(w_o.shape, F32),
                jax.ShapeDtypeStruct((1, dim), F32), jax.ShapeDtypeStruct((1, head_dim), F32),
                jax.ShapeDtypeStruct((1, head_dim), F32)],
            scratch_shapes=[dma((2,)), dma((kv_heads, 5)), dma((3,))],
            compiler_params=pltpu.CompilerParams(vmem_limit_bytes=4 * 1024 * 1024),
            cost_estimate=pl.CostEstimate(flops=10**9, bytes_accessed=60 * 10**6, transcendentals=0),
            name='pack_out',
        )(*[pltpu.with_memory_space_constraint(a, pltpu.VMEM) for a in (y, d_hidden, slices, small)])
        return (y.reshape(hidden.shape), d_hidden.reshape(hidden.shape), d_wq, d_wk, d_wv, d_wo, d_ng[0], d_qg[0], d_kg[0])

    return jax.shard_map(local_step, mesh=mesh, in_specs=(seq_spec, replicated, replicated, replicated, replicated, replicated, replicated, replicated, seq_spec), out_specs=(seq_spec, seq_spec, replicated, replicated, replicated, replicated, replicated, replicated, replicated), check_vma=False)
```

```python
import math
import jax
import jax.numpy as jnp
import numpy as np
from jax import lax
from jax.experimental import pallas as pl
from jax.experimental.pallas import tpu as pltpu
from jax.sharding import PartitionSpec as P

ROPE_BASE = 1000000.0
NORM_EPS = 1e-6
LOG2E = 1.4426950408889634
F32 = jnp.float32
BF16 = jnp.bfloat16
QBLK = 256
OUT_MASKS = (14, 12, 8, 6, 4, 10, 2, 15, 13, 9, 7, 5, 11, 3, 1)
AHEAD = 3
VMEM_LIMIT = 36640 * 1024
COLOURS = ((1, 2, 3), (2, 3, 1), (3, 1, 2))
PER_POINT = 4
MASKS = (8, 4, 2, 12, 10, 6, 14, 9, 5, 3, 13, 11, 7, 15, 1)


def dot(a, b, ca, cb):
    return lax.dot_general(a, b, (((ca,), (cb,)), ((), ())), preferred_element_type=F32)


def rope_tables(n_pos, head_dim):
    half_dim = head_dim // 2
    inv_freq = np.exp(np.arange(half_dim, dtype=np.float32) * np.float32(-2.0 * math.log(ROPE_BASE) / head_dim))
    angles = np.arange(n_pos, dtype=np.float32)[:, None] * inv_freq[None, :]
    cos, sin = np.cos(angles), np.sin(angles)
    return np.concatenate([cos, cos], axis=-1), np.concatenate([-sin, sin], axis=-1)


def norm_rope(raw, gain, cos, sin):
    inv = lax.rsqrt(jnp.mean(raw * raw, axis=-1, keepdims=True) + NORM_EPS)
    unit = raw * inv
    normed = unit * gain
    return normed * cos + pltpu.roll(normed, raw.shape[-1] // 2, 1) * sin, unit, inv


def norm_rope_back(d_rot, unit, inv, gain, cos, sin):
    d_normed = d_rot * cos - pltpu.roll(d_rot, unit.shape[-1] // 2, 1) * sin
    d_gain = jnp.sum(d_normed * unit, axis=0, keepdims=True)
    d_unit = d_normed * gain
    return inv * (d_unit - unit * jnp.mean(d_unit * unit, axis=-1, keepdims=True)), d_gain


def causal_mask_t(scores_t, first_q):
    n_q = scores_t.shape[1]
    key = lax.broadcasted_iota(jnp.int32, (n_q, n_q), 0)
    query = lax.broadcasted_iota(jnp.int32, (n_q, n_q), 1)
    diag = jnp.where(query >= key, scores_t[first_q:], -1e30 * LOG2E)
    if first_q == 0:
        return diag
    return jnp.concatenate([scores_t[:first_q], diag], axis=0)


def block_kernel(n_groups, *refs):
    n_steps = n_groups + 4

    def body(step, carry):
        block_step(step, n_steps, n_groups, *refs)
        return carry
    lax.fori_loop(0, n_steps, body, 0)


def block_step(step, n_steps, n_groups, hid_ref, dyin_ref, gain_ref, wq_ref, wk_ref, wv_ref, wo_ref, qg_ref, kg_ref,
               cos_ref, sin_ref, y_ref, dx_ref, u, small_ref,
               xs, dys, hs, ht, wcats, wos, dqkv, oall, dqkv_early, o_early, y_acc, dn_acc, r0, r1, r2, r3, r4, sm, smr,
               in_send, in_recv, in_loc, d_send, d_recv, p_send, p_recv, g_send, g_recv, e_send, e_recv,
               s_send, s_recv, out_send, out_recv, out_loc, w_sem):
    n_dev, rows, n_loc, dim = hid_ref.shape
    n_pos = n_dev * n_loc
    head_dim = qg_ref.shape[-1]
    qw = wos.shape[1]
    group = qw // head_dim
    width = qw + 2 * head_dim
    half = u.shape[1] // 2
    lane = half // 2
    blk = lane // 3
    me = lax.axis_index('sp')
    bit = [(me // (1 << i)) % 2 for i in range(4)]
    partner = [me + (1 << i) * (1 - 2 * bit[i]) for i in range(4)]

    def remote(src, dst, send, recv, device):
        return pltpu.make_async_remote_copy(src_ref=src, dst_ref=dst, send_sem=send, recv_sem=recv,
                                            device_id=(device,), device_id_type=pl.DeviceIdType.MESH)

    def rows_of(g, start, size):
        return u.at[g, pl.ds(pl.multiple_of(start, 16), size)]

    own = [bit[0] * half + h * lane for h in range(2)]
    other = [(1 - bit[0]) * half + h * lane for h in range(2)]
    keep1, send1, keep2, send2, keep3, send3 = {}, {}, {}, {}, {}, {}
    for h in range(2):
        for c, (d1, d2, d3) in enumerate(COLOURS):
            base = own[h] + c * blk
            keep1[h, c] = base + bit[d1] * (blk // 2)
            send1[h, c] = base + (1 - bit[d1]) * (blk // 2)
            keep2[h, c] = keep1[h, c] + bit[d2] * (blk // 4)
            send2[h, c] = keep1[h, c] + (1 - bit[d2]) * (blk // 4)
            keep3[h, c] = keep2[h, c] + bit[d3] * (blk // 8)
            send3[h, c] = keep2[h, c] + (1 - bit[d3]) * (blk // 8)

    def core_scatter(g, h):
        return remote(rows_of(g, other[h], lane), r0.at[g % 2, h], d_send.at[h, g % 2], d_recv.at[h, g % 2], partner[0])

    def scatter(phase, c, g, h):
        start, size, buf = ((send1, blk // 2, r1), (send2, blk // 4, r2), (send3, blk // 8, r3))[phase]
        return remote(rows_of(g, start[h, c], size), buf.at[g % 2, h, c], p_send.at[phase, c, h, g % 2],
                      p_recv.at[phase, c, h, g % 2], partner[COLOURS[c][phase]])

    def gather(phase, c, g, h):
        start, size = ((keep3, blk // 8), (keep2, blk // 4), (keep1, blk // 2))[phase]
        part = rows_of(g, start[h, c], size)
        return remote(part, part if phase else r4.at[g % 2, h, c], g_send.at[phase, c, h, g % 2],
                      g_recv.at[phase, c, h, g % 2], partner[COLOURS[c][2 - phase]])

    def core_gather(g, h):
        part = rows_of(g, own[h], lane)
        return remote(part, part, e_send.at[h, g % 2], e_recv.at[h, g % 2], partner[0])

    def add_rows(g, start, size, buf):
        s = pl.ds(pl.multiple_of(start, 16), size)
        u[g, s] = u[g, s] + buf

    def stage(k, g, h):
        slot = g % 2
        if k == 1:
            core_scatter(g, h).wait()
            for c in range(3):
                add_rows(g, own[h] + c * blk, blk, r0[slot, h, c * blk:(c + 1) * blk])
                scatter(0, c, g, h).start()
        elif k in (2, 3, 4):
            keep, size, buf = ((keep1, blk // 2, r1), (keep2, blk // 4, r2), (keep3, blk // 8, r3))[k - 2]
            for c in range(3):
                scatter(k - 2, c, g, h).wait()
            for c in range(3):
                add_rows(g, keep[h, c], size, buf[slot, h, c])
                (scatter(k - 1, c, g, h) if k < 4 else gather(0, c, g, h)).start()
        elif k in (5, 6):
            for c in range(3):
                gather(k - 5, c, g, h).wait()
            for c in range(3):
                if k == 5:
                    u[g, pl.ds(pl.multiple_of(send3[h, c], 16), blk // 8)] = r4[slot, h, c]
                gather(k - 4, c, g, h).start()
        elif k == 7:
            for c in range(3):
                gather(2, c, g, h).wait()
            core_gather(g, h).start()
        else:
            core_gather(g, h).wait()

    sends = [(which, row, mask) for row in range(2) for which in (1, 0) for mask in OUT_MASKS]

    def handler(sub):
        h = sub % 2
        for k in range(8, 0, -1):
            if (2 * k - 2 + h - sub) % 4 == 0:
                g = step - 1 - (2 * k - 2 + h - sub) // 4

                @pl.when((g >= 0) & (g < n_groups))
                def _():
                    stage(k, g, h)
        for i in range(5):
            if (2 * i + 3) % 4 == sub:
                @pl.when(step == n_groups + (2 * i + 3) // 4)
                def _():
                    if i == 0:
                        small_copy(0).start()
                    else:
                        small_step(i - 1)
        for j in range(-(-len(sends) // PER_POINT)):
            if (j + 1) % 4 == sub:
                @pl.when(step == n_groups + (j + 1) // 4)
                def _():
                    for which, row, mask in sends[j * PER_POINT:(j + 1) * PER_POINT]:
                        to_peers(out_copy, which, row, (mask,))

    def small_copy(i):
        return remote(sm.at[i], smr.at[i], s_send.at[i], s_recv.at[i], partner[i])

    def small_step(i):
        small_copy(i).wait()
        sm[i + 1] = sm[i] + smr[i]
        if i < 3:
            small_copy(i + 1).start()
        else:
            small_ref[...] = sm[4]

    def in_copy(which, row, peer):
        src, dst = (hid_ref, xs) if which == 0 else (dyin_ref, dys)
        n = 2 * row + which
        return remote(src.at[peer, row], dst.at[row, me], in_send.at[n], in_recv.at[n], peer)

    def in_local(which, row):
        src, dst = (hid_ref, xs) if which == 0 else (dyin_ref, dys)
        return pltpu.make_async_copy(src.at[me, row], dst.at[row, me], in_loc.at[2 * row + which])

    def in_wait(which, row):
        dst = xs if which == 0 else dys
        n = 2 * row + which
        many = dst.at[row, pl.ds(0, n_dev - 1)]
        pltpu.make_async_copy(many, many, in_recv.at[n]).wait()
        in_local(which, row).wait()

    def in_wait_send(which, row):
        many = (xs if which == 0 else dys).at[row, pl.ds(0, n_dev - 1)]
        pltpu.make_async_copy(many, many, in_send.at[2 * row + which]).wait()

    def out_copy(which, row, peer):
        src, dst = (xs, y_ref) if which == 0 else (dys, dx_ref)
        n = 2 * row + which
        return remote(src.at[row, peer], dst.at[me, row], out_send.at[n], out_recv.at[n], peer)

    def out_local(which, row):
        src, dst = (xs, y_ref) if which == 0 else (dys, dx_ref)
        return pltpu.make_async_copy(src.at[row, me], dst.at[me, row], out_loc.at[2 * row + which])

    def to_peers(make, which, row, masks):
        for mask in masks:
            make(which, row, me + sum((mask & (1 << i)) * (1 - 2 * bit[i]) for i in range(4))).start()

    @pl.when(step == 0)
    def _():
        barrier = pltpu.get_barrier_semaphore()

        def greet(d, carry):
            pl.semaphore_signal(barrier, inc=1, device_id=(lax.rem(me + d, n_dev),), device_id_type=pl.DeviceIdType.MESH)
            return carry
        lax.fori_loop(1, n_dev, greet, 0)
        pl.semaphore_wait(barrier, n_dev - 1)
        for row in range(rows):
            for which in range(2):
                in_local(which, row).start()
                to_peers(in_copy, which, row, MASKS)
        y_acc[...] = jnp.zeros_like(y_acc)
        dn_acc[...] = jnp.zeros_like(dn_acc)
        sm[0] = jnp.zeros_like(sm[0])

    def tokens_of(row):
        return slice(row * n_pos, (row + 1) * n_pos)

    def row_compute(row, g, arriving, d_to, o_to):
        tok = tokens_of(row)
        wcat, wo = wcats.at[g % 2], wos.at[g % 2]
        cos, sin = cos_ref[...], sin_ref[...]
        scale = head_dim ** -0.5
        qkv = dot(hs[tok], wcat[...], 1, 0).astype(BF16)

        def grad_heads():
            return dot(dys[row].reshape(n_pos, dim), wo[...], 1, 1).astype(BF16)

        def probs_of(first, q_blk, cols):
            n_key = first + QBLK
            scores = causal_mask_t(dot(k_rot[:n_key], q_blk, 1, 1) * (scale * LOG2E), first)
            e = jnp.exp2(scores - jnp.max(scores, axis=0, keepdims=True))
            prob = e * (1.0 / jnp.sum(e, axis=0, keepdims=True))
            prob_bf = prob.astype(BF16)
            o_to[first:n_key, cols] = dot(prob_bf, v[:n_key], 0, 0).astype(BF16)
            return prob, prob_bf

        k_rot, k_unit, k_inv = norm_rope(qkv[:, qw:qw + head_dim].astype(F32), kg_ref[...], cos, sin)
        k_rot = k_rot.astype(BF16)
        v = qkv[:, qw + head_dim:]
        if arriving:
            early = []
            for j in range(group):
                cols = slice(j * head_dim, (j + 1) * head_dim)
                q_rot, q_unit, q_inv = norm_rope(qkv[:, cols].astype(F32), qg_ref[...], cos, sin)
                q_rot = q_rot.astype(BF16)
                early.append((q_rot, q_unit, q_inv, [probs_of(first, q_rot[first:first + QBLK], cols) for first in range(0, n_pos, QBLK)]))
            in_wait(1, row)
        d_o = grad_heads()
        dk_sum = [jnp.zeros((QBLK, head_dim), F32) for _ in range(n_pos // QBLK)]
        dv_sum = [jnp.zeros((QBLK, head_dim), F32) for _ in range(n_pos // QBLK)]
        for j in range(group):
            cols = slice(j * head_dim, (j + 1) * head_dim)
            if arriving:
                q_rot, q_unit, q_inv, probs = early[j]
            else:
                q_rot, q_unit, q_inv = norm_rope(qkv[:, cols].astype(F32), qg_ref[...], cos, sin)
                q_rot = q_rot.astype(BF16)
            dq_parts = []
            for first in range(0, n_pos, QBLK):
                n_key = first + QBLK
                q_blk = q_rot[first:n_key]
                do_blk = d_o[first:n_key, cols]
                prob, prob_bf = probs[first // QBLK] if arriving else probs_of(first, q_blk, cols)
                d_prob = dot(v[:n_key], do_blk, 1, 1)
                inner = jnp.sum(prob * d_prob, axis=0, keepdims=True)
                d_scores = (prob * (d_prob - inner) * scale).astype(BF16)
                dv_blk = dot(prob_bf, do_blk, 1, 0)
                dk_blk = dot(d_scores, q_blk, 1, 0)
                for i in range(n_key // QBLK):
                    dv_sum[i] += dv_blk[i * QBLK:(i + 1) * QBLK]
                    dk_sum[i] += dk_blk[i * QBLK:(i + 1) * QBLK]
                dq_parts.append(dot(d_scores, k_rot[:n_key], 0, 0))
            dq = jnp.concatenate(dq_parts, axis=0).astype(BF16).astype(F32)
            dq_raw, d_gain = norm_rope_back(dq, q_unit, q_inv, qg_ref[...], cos, sin)
            d_to[:, cols] = dq_raw.astype(BF16)
            sm[0, 1:2, :head_dim] += d_gain
        dk = jnp.concatenate(dk_sum, axis=0).astype(BF16).astype(F32)
        dk_raw, d_gain = norm_rope_back(dk, k_unit, k_inv, kg_ref[...], cos, sin)
        d_to[:, qw:qw + head_dim] = dk_raw.astype(BF16)
        sm[0, 1:2, head_dim:2 * head_dim] += d_gain
        d_to[:, qw + head_dim:] = jnp.concatenate(dv_sum, axis=0).astype(BF16)

    def input_norm(row):
        x = xs[row].reshape(n_pos, dim).astype(F32)
        inv = lax.rsqrt(jnp.mean(x * x, axis=-1, keepdims=True) + NORM_EPS)
        h = (x * inv * gain_ref[...]).astype(BF16)
        hs[tokens_of(row)] = h
        ht[:, tokens_of(row)] = h.T

    def finish_row(row):
        tok = tokens_of(row)
        x = xs[row].reshape(n_pos, dim).astype(F32)
        inv = lax.rsqrt(jnp.mean(x * x, axis=-1, keepdims=True) + NORM_EPS)
        unit = x * inv
        d_normed = dn_acc[tok]
        sm[0, 0:1] += jnp.sum(d_normed * unit, axis=0, keepdims=True)
        d_unit = d_normed * gain_ref[...]
        d_x = inv * (d_unit - unit * jnp.mean(d_unit * unit, axis=-1, keepdims=True))
        d_y = dys[row].reshape(n_pos, dim).astype(F32)
        dys[row] = (d_y + d_x).astype(BF16).reshape(n_dev, n_loc, dim)
        xs[row] = (x + y_acc[tok]).astype(BF16).reshape(n_dev, n_loc, dim)

    computing = step < n_groups

    def weight_copies(g):
        slot = g % 2
        col = lambda n: pl.ds(pl.multiple_of(g * n, 128), n)
        pieces = ((wq_ref.at[:, col(qw)], wcats.at[slot, :, :qw]),
                  (wk_ref.at[:, col(head_dim)], wcats.at[slot, :, qw:qw + head_dim]),
                  (wv_ref.at[:, col(head_dim)], wcats.at[slot, :, qw + head_dim:]),
                  (wo_ref.at[col(qw)], wos.at[slot]))
        return [pltpu.make_async_copy(a, b, w_sem.at[slot, i]) for i, (a, b) in enumerate(pieces)]

    def weights(g, n):
        for copy in weight_copies(g):
            copy.wait()

        @pl.when(g + 1 < n)
        def _():
            for copy in weight_copies(g + 1):
                copy.start()

    @pl.when(step == 0)
    def _():
        for copy in weight_copies(0):
            copy.start()
        in_wait(0, 0)
        input_norm(0)
        in_wait(1, 0)

        def first_row(g, carry):
            weights(g, AHEAD)
            row_compute(0, g, False, dqkv_early.at[g], o_early.at[g])
            return carry
        lax.fori_loop(0, AHEAD, first_row, 0)
        for copy in weight_copies(0):
            copy.start()
        in_wait(0, 1)
        input_norm(1)

    @pl.when(computing)
    def _():
        weights(step, n_groups)

    for row in range(rows):
        handler(row)

        if row == 0:
            @pl.when(step < AHEAD)
            def _():
                dqkv[:n_pos] = dqkv_early[step]
                oall[:n_pos] = o_early[step]

        def into(row, arriving):
            row_compute(row, step, arriving, dqkv.at[tokens_of(row)], oall.at[tokens_of(row)])

        if row == 1:
            @pl.when(step == 0)
            def _():
                into(row, True)

        @pl.when(computing & (step >= (AHEAD if row == 0 else 1)))
        def _():
            into(row, False)

        @pl.when(step == n_groups)
        def _():
            for which in range(2):
                in_wait_send(which, row)
            finish_row(row)
            for which in range(2):
                out_local(which, row).start()

    handler(2)

    @pl.when(computing)
    def _():
        u[step, :dim] = dot(ht[...], dqkv[...], 1, 0)
        d_wo = dot(oall[...], dys[...].reshape(rows * n_pos, dim), 0, 0)
        u[step, dim:dim + qw] = d_wo[:, :width]
        u[step, dim + qw:] = d_wo[:, width:]
        for h in range(2):
            core_scatter(step, h).start()

    handler(3)

    @pl.when(computing)
    def _():
        y_acc[...] += dot(oall[...], wos[step % 2], 1, 0)
        dn_acc[...] += dot(dqkv[...], wcats[step % 2], 1, 1)

    @pl.when(step == n_steps - 1)
    def _():
        for row in range(rows):
            for which in range(2):
                n = 2 * row + which
                many = (xs if which == 0 else dys).at[row, pl.ds(0, n_dev - 1)]
                landed = (y_ref if which == 0 else dx_ref).at[pl.ds(0, n_dev - 1), row]
                pltpu.make_async_copy(many, many, out_send.at[n]).wait()
                pltpu.make_async_copy(landed, landed, out_recv.at[n]).wait()
                out_local(which, row).wait()


def place_kernel(y_in, dx_in, u, small, y_ref, dx_ref, dwq_ref, dwk_ref, dwv_ref, dwo_ref, dg_ref, dqg_ref, dkg_ref,
                 out_sem, w_sem, s_sem):
    dim, head_dim = dg_ref.shape[1], dqg_ref.shape[1]
    n_groups, _, width = u.shape
    qw = dwq_ref.shape[1] // n_groups
    stores = []
    for g in range(n_groups):
        col = lambda n: slice(g * n, (g + 1) * n)
        pieces = ((u.at[g, :dim, :qw], dwq_ref.at[:, col(qw)]),
                  (u.at[g, :dim, qw:qw + head_dim], dwk_ref.at[:, col(head_dim)]),
                  (u.at[g, :dim, qw + head_dim:], dwv_ref.at[:, col(head_dim)]),
                  (u.at[g, dim:dim + qw], dwo_ref.at[col(qw), :width]),
                  (u.at[g, dim + qw:], dwo_ref.at[col(qw), width:]))
        stores += [pltpu.make_async_copy(src, dst, w_sem.at[g, i]) for i, (src, dst) in enumerate(pieces)]
    stores += [pltpu.make_async_copy(src, dst, s_sem.at[i]) for i, (src, dst) in enumerate((
        (small.at[0:1], dg_ref), (small.at[1:2, :head_dim], dqg_ref), (small.at[1:2, head_dim:2 * head_dim], dkg_ref)))]
    stores += [pltpu.make_async_copy(src, dst, out_sem.at[i]) for i, (src, dst) in enumerate(((y_in, y_ref), (dx_in, dx_ref)))]
    for copy in stores:
        copy.start()
    for copy in stores:
        copy.wait()


def solution(mesh):
    n_dev = mesh.shape['sp']
    seq_spec = P(None, 'sp', None)
    replicated = P()

    def local_step(hidden, norm_gain, w_q, w_k, w_v, q_gain, k_gain, w_o, d_out):
        n_batch, n_loc, dim = hidden.shape
        head_dim = q_gain.shape[0]
        kv_heads = w_k.shape[1] // head_dim
        qw = w_q.shape[1] // kv_heads
        width = qw + 2 * head_dim
        rows = n_batch // n_dev
        n_pos = n_loc * n_dev
        tokens = rows * n_pos
        cos, sin = rope_tables(n_pos, head_dim)
        slice_rows = dim + 2 * qw
        lane = slice_rows // 4
        blk = lane // 3
        anywhere = pl.BlockSpec(memory_space=pl.ANY)
        in_vmem = pl.BlockSpec(memory_space=pltpu.VMEM)
        act = (n_dev, rows, n_loc, dim)
        dma = pltpu.SemaphoreType.DMA
        y, d_hidden, slices, small = pl.pallas_call(
            lambda *refs: block_kernel(kv_heads, *refs),
            in_specs=[anywhere, anywhere, in_vmem, anywhere, anywhere, anywhere, anywhere] + [in_vmem] * 4,
            out_specs=[in_vmem] * 4,
            out_shape=[
                pltpu.VMEM(act, BF16), pltpu.VMEM(act, BF16),
                pltpu.VMEM((kv_heads, slice_rows, width), F32), pltpu.VMEM((8, dim), F32)],
            scratch_shapes=[
                pltpu.VMEM((rows, n_dev, n_loc, dim), BF16), pltpu.VMEM((rows, n_dev, n_loc, dim), BF16),
                pltpu.VMEM((tokens, dim), BF16), pltpu.VMEM((dim, tokens), BF16),
                pltpu.VMEM((2, dim, width), BF16), pltpu.VMEM((2, qw, dim), BF16),
                pltpu.VMEM((tokens, width), BF16), pltpu.VMEM((tokens, qw), BF16),
                pltpu.VMEM((AHEAD, n_pos, width), BF16), pltpu.VMEM((AHEAD, n_pos, qw), BF16),
                pltpu.VMEM((tokens, dim), F32), pltpu.VMEM((tokens, dim), F32),
                pltpu.VMEM((2, 2, lane, width), F32), pltpu.VMEM((2, 2, 3, blk // 2, width), F32),
                pltpu.VMEM((2, 2, 3, blk // 4, width), F32), pltpu.VMEM((2, 2, 3, blk // 8, width), F32),
                pltpu.VMEM((2, 2, 3, blk // 8, width), F32),
                pltpu.VMEM((5, 8, dim), F32), pltpu.VMEM((4, 8, dim), F32),
                dma((4,)), dma((4,)), dma((4,)), dma((2, 2)), dma((2, 2)), dma((3, 3, 2, 2)), dma((3, 3, 2, 2)),
                dma((3, 3, 2, 2)), dma((3, 3, 2, 2)), dma((2, 2)), dma((2, 2)), dma((4,)), dma((4,)),
                dma((4,)), dma((4,)), dma((4,)), dma((2, 4))],
            compiler_params=pltpu.CompilerParams(
                vmem_limit_bytes=VMEM_LIMIT, collective_id=0, has_side_effects=True),
            cost_estimate=pl.CostEstimate(flops=52 * 10**9, bytes_accessed=50 * 10**6, transcendentals=0),
            name='attn_block',
        )(hidden.reshape(act), d_out.reshape(act), norm_gain[None], w_q, w_k, w_v, w_o, q_gain[None], k_gain[None],
          jnp.asarray(cos), jnp.asarray(sin))
        y, d_hidden, d_wq, d_wk, d_wv, d_wo, d_ng, d_qg, d_kg = pl.pallas_call(
            place_kernel,
            in_specs=[in_vmem] * 4,
            out_specs=[anywhere] * 9,
            out_shape=[
                jax.ShapeDtypeStruct(act, BF16), jax.ShapeDtypeStruct(act, BF16),
                jax.ShapeDtypeStruct(w_q.shape, F32), jax.ShapeDtypeStruct(w_k.shape, F32),
                jax.ShapeDtypeStruct(w_v.shape, F32), jax.ShapeDtypeStruct(w_o.shape, F32),
                jax.ShapeDtypeStruct((1, dim), F32), jax.ShapeDtypeStruct((1, head_dim), F32),
                jax.ShapeDtypeStruct((1, head_dim), F32)],
            scratch_shapes=[dma((2,)), dma((kv_heads, 5)), dma((3,))],
            compiler_params=pltpu.CompilerParams(vmem_limit_bytes=4 * 1024 * 1024),
            cost_estimate=pl.CostEstimate(flops=10**9, bytes_accessed=60 * 10**6, transcendentals=0),
            name='pack_out',
        )(*[pltpu.with_memory_space_constraint(a, pltpu.VMEM) for a in (y, d_hidden, slices, small)])
        return (y.reshape(hidden.shape), d_hidden.reshape(hidden.shape), d_wq, d_wk, d_wv, d_wo, d_ng[0], d_qg[0], d_kg[0])

    return jax.shard_map(local_step, mesh=mesh, in_specs=(seq_spec, replicated, replicated, replicated, replicated, replicated, replicated, replicated, seq_spec), out_specs=(seq_spec, seq_spec, replicated, replicated, replicated, replicated, replicated, replicated, replicated), check_vma=False)
```
